32 devices in a mesh: kgrp: 2 (over y), pw: 4 (over z), band: 4 (over x, core).
Axes of the slice: x: 2, y: 2, z: 4, core: 2. Of those that a mesh axis runs over, the one named last changes fastest.
Arguments:
- waves: float32 [128, 4, 16, 256], P('band', 'kgrp', 'pw'), parts along dimension 1, as said below
- forward: float32 [128, 4, 16, 256], P('band', 'kgrp', 'pw'), parts along dimension 1, as said below
- backward: float32 [128, 4, 16, 256], P('band', 'kgrp', 'pw'), parts along dimension 1, as said below
- projectors: float32 [256, 2, 16, 256], P('kgrp', None, 'pw'), parts along dimension 0, as said below
- potential: float32 [256, 16], P('pw'), may hold values from 0.25 to 2
- strengths: float32 [128], replicated, may hold values from 0.5 to 4
- shifts: float32 [128], P('band'), may hold values from 0.5 to 2
Outputs:
- response: float32 [128, 4, 16, 256], P('band', 'kgrp', 'pw'), parts along dimension 1
- derivative: float32 [128, 4, 16, 256], P('band', 'kgrp', 'pw'), parts along dimension 1
The draws below stay inside these ranges and needn't reach their ends.
There are 2 independent parts, one for each index of `kgrp`. The reference program is written for one: setup_inputs(seed, part) draws one part's arguments, and reference() takes and returns one part's arrays. A program takes and returns all parts, laid end to end along the dimension named above; an argument that names none is the same for every part. Nothing has to cross between parts.
Inputs may be any that keep to these rules, and one draw needn't show every extreme that they name: `waves`: real and imaginary parts of every band's coefficients are drawn independently at every grid point. `forward`: the margin of the slab's bands with these coefficients is an invertible matrix. `backward`: the margin of the slab's bands with these coefficients is an invertible matrix. `projectors`: real and imaginary parts of every projector are drawn independently at every grid point.
All inputs are finite; a program needn't handle non-finite values.
Results may differ from the reference program's by a relative error of at most 0.0003.
Values sent between devices are 32-bit elements; how exact they have to be, the bound alone decides.
A program may use at most 64 MiB of HBM per device.

```python
import math
import jax
import jax.numpy as jnp
from jax import lax

SLAB = 128
NPROJ = 128
F2 = 256
ITERS = 2
F1 = 16


precise = lax.Precision.HIGHEST


def combine_drawn(vectors, coeffs):
    table = jnp.stack([jnp.stack([coeffs[0], coeffs[1]]), jnp.stack([-coeffs[1], coeffs[0]])])
    return jnp.einsum('ixg,xyij->jyg', vectors, table, precision=precise)


def rough(key, count_rows):
    shape = (count_rows, 2, F1 * F2)
    values = jnp.clip(jax.random.normal(key, shape, jnp.float32), -6.0, 6.0) * 0.70710677
    return values


def neighbour(base, wave_flat, projector_flat):
    mixing = jax.random.normal(jax.random.fold_in(base, 1), (2, SLAB, SLAB), jnp.float32) * (0.2 / math.sqrt(2.0 * SLAB))
    mixing = mixing.at[0].add(jnp.eye(SLAB, dtype=jnp.float32))
    coeffs = jax.random.normal(jax.random.fold_in(base, 2), (2, NPROJ, SLAB), jnp.float32) * (0.70710677 / math.sqrt(NPROJ))
    noise = (rough(jax.random.fold_in(base, 3), SLAB) + combine_drawn(projector_flat, coeffs)) * 0.70710677
    return combine_drawn(wave_flat, mixing) + 0.1 * noise


def joint(key):
    projector_flat = rough(jax.random.fold_in(key, 101), NPROJ)
    wave_flat = rough(jax.random.fold_in(key, 102), SLAB)
    ahead = neighbour(jax.random.fold_in(key, 104), wave_flat, projector_flat)
    behind = neighbour(jax.random.fold_in(key, 105), wave_flat, projector_flat)
    return (wave_flat.reshape(SLAB, 2, F1, F2), ahead.reshape(SLAB, 2, F1, F2), behind.reshape(SLAB, 2, F1, F2), projector_flat.reshape(NPROJ, 2, F1, F2))


def draw_waves(key, part):
    return joint(key)[0]


def draw_forward(key, part):
    return joint(key)[1]


def draw_backward(key, part):
    return joint(key)[2]


def draw_projectors(key, part):
    return joint(key)[3]


def block_levels(own_key, extent, split, least, high):
    def one(position, blocks):
        draws = jax.random.uniform(jax.random.fold_in(jax.random.fold_in(own_key, 6), position), (blocks,), jnp.float32, least / len(split), high / len(split))
        return jnp.repeat(jnp.exp(draws), extent[position] // blocks).reshape((-1,) + (1,) * (len(extent) - position - 1))

    loudness = one(*split[0])
    for cut in split[1:]:
        loudness = loudness * one(*cut)
    return loudness


def setup_inputs(seed: int = 0, part: int = 0) -> dict:
    arg_keys = jax.random.split(jax.random.key(seed), 8)
    own_keys = jax.random.split(jax.random.fold_in(arg_keys[7], part), 8)
    return {
        "waves": draw_waves(jax.random.fold_in(jax.random.fold_in(arg_keys[7], part), 71), part),
        "forward": draw_forward(jax.random.fold_in(jax.random.fold_in(arg_keys[7], part), 71), part),
        "backward": draw_backward(jax.random.fold_in(jax.random.fold_in(arg_keys[7], part), 71), part),
        "projectors": draw_projectors(jax.random.fold_in(jax.random.fold_in(arg_keys[7], part), 71), part),
        "potential": jnp.clip(0.25 + 1.75 * jax.random.uniform(arg_keys[4], (F2, F1), jnp.float32) ** block_levels(arg_keys[4], (F2, F1), ((0, 4),), -0.2, 0.2), 0.25, 2.0),
        "strengths": jnp.clip(jnp.exp(jax.random.uniform(arg_keys[5], (NPROJ,), jnp.float32, math.log(0.5), math.log(4.0))), 0.5, 4.0),
        "shifts": jnp.clip(jnp.exp(math.log(2.0) - 1.3862944 * jax.random.uniform(arg_keys[6], (SLAB,), jnp.float32) ** block_levels(arg_keys[6], (SLAB,), ((0, 4),), -0.2, 0.2)), 0.5, 2.0),
    }


precise = lax.Precision.HIGHEST
string_step = 0.05
kinetic_scale = 4.0

def margin(left_set, right_set):
    products = jnp.einsum('ixg,jyg->xyij', left_set, right_set, precision=precise)
    return jnp.stack([products[0, 0] + products[1, 1], products[0, 1] - products[1, 0]])

def combine(vectors, coeffs):
    table = jnp.stack([jnp.stack([coeffs[0], coeffs[1]]), jnp.stack([-coeffs[1], coeffs[0]])])
    return jnp.einsum('ixg,xyij->jyg', vectors, table, precision=precise)

def invert(matrix):
    real_part = matrix[0]
    imag_part = matrix[1]
    embedded = jnp.concatenate([jnp.concatenate([real_part, -imag_part], 1), jnp.concatenate([imag_part, real_part], 1)], 0)
    normal = jnp.dot(embedded.T, embedded, precision=precise)
    lower_factor = jnp.linalg.cholesky(normal)
    middle = lax.linalg.triangular_solve(lower_factor, embedded.T, left_side=True, lower=True)
    inverse = lax.linalg.triangular_solve(lower_factor, middle, left_side=True, lower=True, transpose_a=True)
    count_rows = real_part.shape[0]
    return jnp.stack([inverse[:count_rows, :count_rows], inverse[count_rows:, :count_rows]])

def centred(index, length):
    shifted = (index + length // 2) % length - length // 2
    return shifted.astype(jnp.float32) / length

def smooth_term(vectors, potential):
    field = lax.complex(vectors[:, 0], vectors[:, 1])
    real_space = jnp.fft.ifft2(field) * potential.T[None]
    returned = jnp.fft.fft2(real_space)
    return jnp.stack([jnp.real(returned), jnp.imag(returned)], axis=1)

def operate(direction, potential, projector_flat, strengths, diagonal):
    count_bands = direction.shape[0]
    points = F1 * F2
    coupling = margin(projector_flat, direction.reshape(count_bands, 2, points)) / points
    nonlocal_part = combine(projector_flat, coupling * strengths[None, :, None]).reshape(direction.shape)
    return diagonal * direction + smooth_term(direction, potential) + nonlocal_part

def reference(waves, forward, backward, projectors, potential, strengths, shifts):
    points = F1 * F2
    waves_flat = waves.reshape(SLAB, 2, points)
    forward_flat = forward.reshape(SLAB, 2, points)
    backward_flat = backward.reshape(SLAB, 2, points)
    forward_margin = margin(waves_flat, forward_flat) / points
    backward_margin = margin(waves_flat, backward_flat) / points
    forward_inverse = invert(forward_margin)
    backward_inverse = invert(backward_margin)
    moved = combine(forward_flat, forward_inverse) - combine(backward_flat, backward_inverse)
    derivative = (moved / (2.0 * string_step)).reshape(SLAB, 2, F1, F2)
    first_index = jnp.arange(F1, dtype=jnp.int32)
    second_index = jnp.arange(F2, dtype=jnp.int32)
    first_freq = centred(first_index, F1)
    second_freq = centred(second_index, F2)
    kinetic = kinetic_scale * (first_freq[:, None] * first_freq[:, None] + second_freq[None, :] * second_freq[None, :])
    diagonal = kinetic[None, None] + shifts[:, None, None, None]
    projector_flat = projectors.reshape(NPROJ, 2, points)
    residual = -derivative
    direction = residual
    solution = jnp.zeros_like(residual)
    norm_now = jnp.sum(residual * residual, axis=(1, 2, 3))
    for turn in range(ITERS):
        image = operate(direction, potential, projector_flat, strengths, diagonal)
        curvature = jnp.sum(direction * image, axis=(1, 2, 3))
        alpha = (norm_now / curvature)[:, None, None, None]
        solution = solution + alpha * direction
        if turn + 1 < ITERS:
            residual = residual - alpha * image
            norm_next = jnp.sum(residual * residual, axis=(1, 2, 3))
            direction = residual + (norm_next / norm_now)[:, None, None, None] * direction
            norm_now = norm_next
    return (solution, derivative)
```

```python
import functools
import math

import jax
import jax.numpy as jnp
import numpy as np
from jax import lax
from jax.experimental import pallas as pl
from jax.experimental.pallas import tpu as pltpu
from jax.sharding import PartitionSpec as P

ITERS = 2


precise = lax.Precision.HIGHEST
string_step = 0.05
kinetic_scale = 4.0


def margin(left_set, right_set):
    products = jnp.einsum("ixg,jyg->xyij", left_set, right_set, precision=precise)
    return jnp.stack([products[0, 0] + products[1, 1], products[0, 1] - products[1, 0]])


def combine(vectors, coeffs):
    table = jnp.stack([jnp.stack([coeffs[0], coeffs[1]]), jnp.stack([-coeffs[1], coeffs[0]])])
    return jnp.einsum("ixg,xyij->jyg", vectors, table, precision=precise)


def invert(matrix):
    real_part = matrix[0]
    imag_part = matrix[1]
    embedded = jnp.concatenate(
        [jnp.concatenate([real_part, -imag_part], 1), jnp.concatenate([imag_part, real_part], 1)], 0
    )
    normal = jnp.dot(embedded.T, embedded, precision=precise)
    lower_factor = jnp.linalg.cholesky(normal)
    middle = lax.linalg.triangular_solve(lower_factor, embedded.T, left_side=True, lower=True)
    inverse = lax.linalg.triangular_solve(
        lower_factor, middle, left_side=True, lower=True, transpose_a=True
    )
    count_rows = real_part.shape[0]
    return jnp.stack([inverse[:count_rows, :count_rows], inverse[count_rows:, :count_rows]])


def centred(index, length):
    shifted = (index + length // 2) % length - length // 2
    return shifted.astype(jnp.float32) / length


def dft_table(length, sign):
    index = jnp.arange(length, dtype=jnp.int32)
    phase = index[:, None] * index[None, :] % length
    angle = phase.astype(jnp.float32) * (2.0 * math.pi / length)
    cosine = jnp.cos(angle) / math.sqrt(length)
    sine = sign * jnp.sin(angle) / math.sqrt(length)
    return jnp.stack([jnp.stack([cosine, sine]), jnp.stack([-sine, cosine])])


def body(waves, forward, backward, projectors, potential, strengths, shifts):
    bands = waves.shape[0]
    rows = waves.shape[2]
    width = waves.shape[3]
    peers = lax.axis_size("pw")
    length = rows * peers
    points = float(length * width)
    cells = rows * width
    quarter = width // peers
    waves_flat = waves.reshape(bands, 2, cells)
    forward_flat = forward.reshape(bands, 2, cells)
    backward_flat = backward.reshape(bands, 2, cells)
    offset = lax.axis_index("band") * bands
    every_wave = lax.all_gather(waves_flat, "band", axis=0, tiled=True)
    forward_part = margin(every_wave, forward_flat) / points
    backward_part = margin(every_wave, backward_flat) / points
    forward_part, backward_part = lax.psum((forward_part, backward_part), "pw")
    forward_whole, backward_whole = (
        lax.all_gather(forward_part, "band", axis=2, tiled=True),
        lax.all_gather(backward_part, "band", axis=2, tiled=True),
    )
    forward_inverse = invert(forward_whole)
    backward_inverse = -invert(backward_whole)
    forward_cols = lax.dynamic_slice_in_dim(forward_inverse, offset, bands, 2)
    backward_cols = lax.dynamic_slice_in_dim(backward_inverse, offset, bands, 2)
    moved = combine(
        lax.all_gather(forward_flat, "band", axis=0, tiled=True), forward_cols
    ) + combine(lax.all_gather(backward_flat, "band", axis=0, tiled=True), backward_cols)
    derivative = (moved / (2.0 * string_step)).reshape(bands, 2, rows, width)
    first_index = lax.axis_index("pw") * rows + jnp.arange(rows, dtype=jnp.int32)
    second_index = jnp.arange(width, dtype=jnp.int32)
    first_freq = centred(first_index, length)
    second_freq = centred(second_index, width)
    kinetic = kinetic_scale * (
        first_freq[:, None] * first_freq[:, None] + second_freq[None, :] * second_freq[None, :]
    )
    diagonal = kinetic[None, None] + shifts[:, None, None, None]
    width_out = dft_table(width, 1.0)
    width_back = dft_table(width, -1.0)
    long_out = dft_table(length, 1.0).reshape(2, 2, peers, rows, length)
    long_back = dft_table(length, -1.0).reshape(2, 2, length, peers, rows)
    projector_flat = projectors.reshape(projectors.shape[0], 2, cells)
    residual = -derivative
    direction = residual
    solution = jnp.zeros_like(residual)
    norm_now = lax.psum(jnp.sum(residual * residual, axis=(1, 2, 3)), "pw")
    for turn in range(ITERS):
        sectioned = jnp.einsum("bxrj,xyjk->ykrb", direction, width_out, precision=precise).reshape(
            2, width, rows * bands
        )
        arrived = lax.all_to_all(sectioned, "pw", split_axis=1, concat_axis=2, tiled=True).reshape(
            2, quarter, peers, rows, bands
        )
        field = jnp.einsum("xqsrb,xysrk->yqbk", arrived, long_out, precision=precise)
        weighted = field * potential[None, :, None, :]
        leaving = jnp.einsum("xqbk,xyksr->yqsrb", weighted, long_back, precision=precise).reshape(
            2, quarter, peers * rows * bands
        )
        returned = lax.all_to_all(leaving, "pw", split_axis=2, concat_axis=1, tiled=True).reshape(
            2, width, rows, bands
        )
        smooth_part = jnp.einsum("xkrb,xykj->byrj", returned, width_back, precision=precise)
        coupling = margin(projector_flat, direction.reshape(bands, 2, cells)) / points
        own_energy = jnp.sum(diagonal * direction * direction, axis=(1, 2, 3)) + jnp.sum(
            weighted * field, axis=(0, 1, 3)
        )
        coupling, own_energy = lax.psum((coupling, own_energy), "pw")
        nonlocal_part = combine(projector_flat, coupling * strengths[None, :, None]).reshape(
            direction.shape
        )
        image = diagonal * direction + smooth_part + nonlocal_part
        curvature = own_energy + points * jnp.sum(
            strengths[None, :, None] * coupling * coupling, axis=(0, 1)
        )
        image, curvature = (image, curvature)
        alpha = (norm_now / curvature)[:, None, None, None]
        solution = solution + alpha * direction
        if turn + 1 < ITERS:
            residual = residual - alpha * image
            norm_next = lax.psum(jnp.sum(residual * residual, axis=(1, 2, 3)), "pw")
            direction = residual + (norm_next / norm_now)[:, None, None, None] * direction
            norm_now = norm_next
    return (solution, derivative)


MESH = pl.DeviceIdType.MESH
TILE = 8


def halves(x):
    high = x.astype(jnp.bfloat16)
    return high, (x - high.astype(jnp.float32)).astype(jnp.bfloat16)


def mul(a, b, turned=False):
    dims = (((1,), (1 if turned else 0,)), ((), ()))
    return lax.dot_general(a, b, dims, preferred_element_type=jnp.float32)


def mul3(a, b, turned=False):
    return mul(a[0], b[0], turned) + (mul(a[0], b[1], turned) + mul(a[1], b[0], turned))


def exact(a, b):
    return jnp.dot(a, b, precision=precise, preferred_element_type=jnp.float32)


def local_plan_fits(args, mesh):
    waves, projectors = args[0], args[3]
    peers, groups = mesh.shape["pw"], mesh.shape["band"]
    bands, rows, width = waves.shape[0], waves.shape[2], waves.shape[3]
    return (
        groups == 4
        and rows == groups
        and bands == TILE * peers
        and bands * groups == 128
        and projectors.shape[0] == 128
        and peers * rows == 16
        and width % 128 == 0
        and projectors.size * peers * 4 <= 8 << 20
    )


def local_kernel(
    peers, groups, sets, proj, pot, strengths, shifts, right_hi, right_lo, left_hi, left_lo,
    resp, deriv,
    got, marg, parts, whole, inv, both, made, field, answer, far, phi, plo, levels,
    s_send, s_recv, r_send, r_recv, g_send, g_recv, t_send, t_recv,
    p1_send, p1_recv, p2_send, p2_recv, p3_send, p3_recv, v_send, v_recv,
    x_send, x_recv, d_send, d_recv, o_send, o_recv,
):
    kgrp = lax.axis_index("kgrp")
    p = lax.axis_index("pw")
    b = lax.axis_index("band")
    core = lax.rem(b, 2)
    side = b // 2
    total = peers * groups
    mine = p * groups + b
    slot = p * 2 + side
    width = sets.shape[4]
    slab = groups * sets.shape[3]
    points = float(total * width)
    barrier = pltpu.get_barrier_semaphore()

    def flat(o):
        q = lax.rem(mine + o, total)
        return q // groups, lax.rem(q, groups)

    for o in range(1, total):
        q, c = flat(o)
        pl.semaphore_signal(barrier, inc=1, device_id=(kgrp, q, c), device_id_type=MESH)
    pl.semaphore_wait(barrier, total - 1)

    started = []

    def send(source, target, ssem, rsem, q, c):
        copy = pltpu.make_async_remote_copy(
            src_ref=source, dst_ref=target, send_sem=ssem, recv_sem=rsem,
            device_id=(kgrp, q, c), device_id_type=MESH,
        )
        copy.start()
        started.append(copy)
        return copy

    first = []
    for a in range(3):
        for o in range(1, groups):
            c = lax.rem(b + o, groups)
            k = a * groups + o
            first.append(send(sets.at[a, c], got.at[a, b], s_send.at[k], s_recv.at[k], p, c))
    pots, pass1 = [], []
    for o in range(1, peers):
        q = lax.rem(p + o, peers)
        pots.append(send(pot, levels.at[p], v_send.at[o], v_recv.at[o], q, b))
    for o in range(1, peers):
        q = lax.rem(p + o, peers)
        pass1.append(send(proj.at[b], far.at[mine], p1_send.at[o], p1_recv.at[o], q, b))
    for a in range(3):
        got[a, b] = sets[a, b]
    levels[p] = pot[...]

    def set_of(a):
        return got[a, :, 0].reshape(slab, width), got[a, :, 1].reshape(slab, width)

    for copy in first[:3]:
        copy.wait_recv()
    wr, wi = set_of(0)
    lhs = halves(
        jnp.concatenate(
            [jnp.concatenate([wr, wi], 1), jnp.concatenate([-wi, wr], 1)], 0
        )
        * (1.0 / points)
    )
    for m in range(2):
        for copy in first[3 * m + 3 : 3 * m + 6]:
            copy.wait_recv()
        fr, fi = set_of(m + 1)
        part = mul3(lhs, halves(jnp.concatenate([fr, fi], 1)), True)
        marg[m] = part.reshape(marg.shape[1:])
    second = []
    for o in range(1, total):
        q, c = flat(o)
        second.append(
            send(marg.at[lax.rem(c, 2), q * 2 + c // 2], parts.at[mine], r_send.at[o], r_recv.at[o], q, c)
        )
    parts[mine] = marg[core, slot]
    def own_rows(r, carry):
        hi, lo = halves(proj[r])
        phi[p * groups + r] = hi
        plo[p * groups + r] = lo
        return carry

    lax.fori_loop(0, groups, own_rows, 0)
    for copy in second:
        copy.wait_recv()
    summed = parts[0]
    for k in range(1, total):
        summed = summed + parts[k]
    whole[slot] = summed
    third = []
    size = total // 2
    for o in range(1, size):
        s = lax.rem(slot + o, size)
        third.append(
            send(whole.at[slot], whole.at[slot], g_send.at[o], g_recv.at[o], s // 2, lax.rem(s, 2) * 2 + core)
        )
    for copy in pass1:
        copy.wait_recv()
    across = lax.rem(b + 2, groups)
    pass2 = []
    for o in range(1, peers):
        row = lax.rem(p + o, peers) * groups + b
        pass2.append(send(far.at[row], far.at[row], p2_send.at[o], p2_recv.at[o], p, across))
    for copy in third:
        copy.wait_recv()
    stacked = whole[...].reshape(2 * slab, slab)
    ar, ai = stacked[:slab], stacked[slab:]
    turned = stacked.T
    inv[0] = exact(turned, stacked)
    inv[1] = exact(turned, jnp.concatenate([ai, -ar], 0))
    lane = lax.broadcasted_iota(jnp.int32, (slab, slab), 1)
    line = lax.broadcasted_iota(jnp.int32, (slab, slab), 0)
    lane1 = lax.broadcasted_iota(jnp.int32, (1, slab), 1)
    line1 = lax.broadcasted_iota(jnp.int32, (slab, 1), 0)

    def eliminate(k, carry):
        nr, ni = inv[0], inv[1]
        rr, ri = inv[0, pl.ds(k, 1), :], inv[1, pl.ds(k, 1), :]
        hit = lane == k
        cr = jnp.sum(jnp.where(hit, nr, 0.0), 1, keepdims=True)
        ci = jnp.sum(jnp.where(hit, ni, 0.0), 1, keepdims=True)
        own = lane1 == k
        scale = 1.0 / jnp.sum(jnp.where(own, rr, 0.0), 1, keepdims=True)
        sr = jnp.where(own, 1.0, rr) * scale
        si = jnp.where(own, 0.0, ri) * scale
        cr = jnp.where(line1 == k, -1.0, cr)
        ci = jnp.where(line1 == k, 0.0, ci)
        gone = jnp.logical_or(hit, line == k)
        inv[0] = jnp.where(gone, 0.0, nr) - (cr * sr - ci * si)
        inv[1] = jnp.where(gone, 0.0, ni) - (cr * si + ci * sr)
        return carry

    lax.fori_loop(0, slab, eliminate, 0)
    kr, ki = inv[0], inv[1]
    mixed = exact(
        jnp.concatenate([jnp.concatenate([ar, -ai], 1), jnp.concatenate([-ai, -ar], 1)], 0),
        jnp.concatenate([kr, ki], 0),
    )
    sign = (1 - 2 * core).astype(jnp.float32) / (2.0 * string_step)
    both[core] = mixed * sign
    sibling = side * 2 + 1 - core
    swap = send(both.at[core], both.at[core], t_send, t_recv, p, sibling)
    for copy in pass2:
        copy.wait_recv()
    pass3 = []
    for o in range(1, peers):
        for j in range(2):
            row = lax.rem(p + o, peers) * groups + (b if j == 0 else across)
            k = 2 * o + j
            pass3.append(send(far.at[row], far.at[row], p3_send.at[k], p3_recv.at[k], p, sibling))
    fr, fi = set_of(1)
    br, bi = set_of(2)
    rhs = halves(jnp.concatenate([fr, fi, br, bi], 0))
    swap.wait_recv()
    f, g = both[0], both[1]
    tfr, tfi, tbr, tbi = f[:slab], f[slab:], g[:slab], g[slab:]
    table = halves(
        jnp.concatenate(
            [
                jnp.concatenate([tfr, -tfi, tbr, -tbi], 1),
                jnp.concatenate([tfi, tfr, tbi, tbr], 1),
            ],
            0,
        )
    )
    made[...] = mul3(table, rhs).reshape(made.shape)
    fields, outs = [], []
    for o in range(1, total):
        q, c = flat(o)
        rows = pl.ds(pl.multiple_of((c * peers + q) * TILE, TILE), TILE)
        fields.append(send(made.at[:, rows], field.at[:, mine], x_send.at[o], x_recv.at[o], q, c))
    span = slab // groups
    for o in range(1, groups):
        c = lax.rem(b + o, groups)
        rows = pl.ds(pl.multiple_of(c * span, TILE), span)
        outs.append(send(made.at[:, rows], deriv.at[b], d_send.at[o], d_recv.at[o], p, c))
    field[:, mine] = made[:, pl.ds(pl.multiple_of((b * peers + p) * TILE, TILE), TILE)]
    deriv[b] = made[:, pl.ds(pl.multiple_of(b * span, TILE), span)]
    for copy in pass3:
        copy.wait_recv()

    def far_rows(t, carry):
        row = lax.rem(p * groups + groups + t, total)
        hi, lo = halves(far[row])
        phi[row] = hi
        plo[row] = lo
        return carry

    lax.fori_loop(0, total - groups, far_rows, 0)
    for copy in pots:
        copy.wait_recv()
    share = width // peers
    level = jnp.concatenate([levels[k][:, :share] for k in range(peers)], 1)
    level = jnp.broadcast_to(level[:, None, :], (total, TILE, width)).reshape(total * TILE, width)
    iu = lax.broadcasted_iota(jnp.int32, (total, TILE, width), 0)
    iw = lax.broadcasted_iota(jnp.int32, (total, TILE, width), 2)
    fu = jnp.where(iu < total // 2, iu, iu - total).astype(jnp.float32) / total
    fw = jnp.where(iw < width // 2, iw, iw - width).astype(jnp.float32) / width
    shift = shifts[pl.ds(pl.multiple_of(p * TILE, TILE), TILE), :]
    diagonal = kinetic_scale * (fu * fu + fw * fw) + shift[None]
    diagonal = diagonal.reshape(total * TILE, width)
    scale = strengths[...] * (1.0 / points)
    for copy in fields:
        copy.wait_recv()

    def transform(xr, xi):
        y = mul3(halves(jnp.concatenate([xr, xi], 1)), (right_hi[...], right_lo[...]))
        y = jnp.concatenate([y[:, :width], y[:, width:]], 0)
        z = mul3((left_hi[...], left_lo[...]), halves(y))
        return z[: total * TILE], z[total * TILE :]

    def operate(dr, di):
        yr, yi = transform(dr, di)
        zr, zi = transform(yr * level, -(yi * level))
        accr = jnp.zeros((2 * TILE, slab), jnp.float32)
        acci = jnp.zeros((2 * TILE, slab), jnp.float32)
        for i in range(total):
            at = slice(i * TILE, i * TILE + TILE)
            hi, lo = halves(jnp.concatenate([dr[at], di[at]], 0))
            accr = accr + mul3((hi, lo), (phi[i, 0], plo[i, 0]), True)
            acci = acci + mul3((hi, lo), (phi[i, 1], plo[i, 1]), True)
        coupling = jnp.concatenate(
            [accr[:TILE] + acci[TILE:], accr[TILE:] - acci[:TILE]], 0
        ) * scale
        c2 = halves(coupling)
        outr, outi = [], []
        for i in range(total):
            ur = mul3(c2, (phi[i, 0], plo[i, 0]))
            ui = mul3(c2, (phi[i, 1], plo[i, 1]))
            outr.append(ur[:TILE] - ui[TILE:])
            outi.append(ui[:TILE] + ur[TILE:])
        return (
            diagonal * dr + zr + jnp.concatenate(outr, 0),
            diagonal * di - zi + jnp.concatenate(outi, 0),
        )

    def summed_over(x):
        x = x.reshape(total, TILE, width)
        return jnp.sum(jnp.sum(x, 0), 1, keepdims=True)

    def spread(x):
        return jnp.broadcast_to(x[None], (total, TILE, width)).reshape(total * TILE, width)

    rr = -field[0].reshape(total * TILE, width)
    ri = -field[1].reshape(total * TILE, width)
    dr, di = rr, ri
    norm_now = summed_over(rr * rr + ri * ri)
    solr, soli = jnp.zeros_like(dr), jnp.zeros_like(di)
    for turn in range(ITERS):
        imr, imi = operate(dr, di)
        curvature = summed_over(dr * imr + di * imi)
        alpha = spread(norm_now / curvature)
        solr, soli = solr + alpha * dr, soli + alpha * di
        if turn + 1 < ITERS:
            rr, ri = rr - alpha * imr, ri - alpha * imi
            norm_next = summed_over(rr * rr + ri * ri)
            beta = spread(norm_next / norm_now)
            dr, di = rr + beta * dr, ri + beta * di
            norm_now = norm_next
    answer[0] = solr.reshape(total, TILE, width)
    answer[1] = soli.reshape(total, TILE, width)
    here = pl.ds(pl.multiple_of(p * TILE, TILE), TILE)
    for o in range(1, peers):
        q = lax.rem(p + o, peers)
        outs.append(
            send(answer.at[:, pl.ds(q * groups, groups)], resp.at[:, :, here], o_send.at[o], o_recv.at[o], q, b)
        )
    resp[:, :, here] = answer[:, pl.ds(p * groups, groups)]
    for copy in outs:
        copy.wait_recv()
    for copy in started:
        copy.wait_send()


def tables(length, repeat):
    index = np.arange(length)
    angle = (index[:, None] * index[None, :] % length) * (2.0 * math.pi / length)
    eye = np.eye(repeat)
    cosine = np.kron(np.cos(angle) / math.sqrt(length), eye)
    sine = np.kron(np.sin(angle) / math.sqrt(length), eye)
    return cosine.astype(np.float32), sine.astype(np.float32)


def split_table(table):
    return halves(jnp.asarray(table))


def local_body(mesh, waves, forward, backward, projectors, potential, strengths, shifts):
    peers, groups = mesh.shape["pw"], mesh.shape["band"]
    bands, _, rows, width = waves.shape
    slab, total = bands * groups, peers * rows
    sets = jnp.stack([waves, forward, backward]).transpose(0, 3, 2, 1, 4)
    proj = projectors.transpose(2, 1, 0, 3)
    pot = jnp.pad(potential.T, ((0, 0), (0, 128 - potential.shape[0] % 128)))
    c, s = tables(width, 1)
    right = split_table(np.block([[c, s], [-s, c]]))
    c, s = tables(total, TILE)
    left = split_table(np.block([[c, -s], [s, c]]))
    f32 = jnp.float32
    dma = pltpu.SemaphoreType.DMA
    vmem = pl.BlockSpec(memory_space=pltpu.VMEM)
    sems = []
    for count in (3 * groups, total, total // 2):
        sems += [dma((count,)), dma((count,))]
    sems += [dma, dma]
    for count in (peers, peers, 2 * peers, peers, total, groups, peers):
        sems += [dma((count,)), dma((count,))]
    resp, deriv = pl.pallas_call(
        functools.partial(local_kernel, peers, groups),
        out_shape=(
            jax.ShapeDtypeStruct((2, rows, bands, width), f32),
            jax.ShapeDtypeStruct((rows, 2, bands, width), f32),
        ),
        in_specs=[vmem] * 9,
        out_specs=(vmem, vmem),
        scratch_shapes=[
            pltpu.VMEM((3, groups, 2, bands, width), f32),
            pltpu.VMEM((2, total // 2, 4 * slab // total, slab), f32),
            pltpu.VMEM((total, 4 * slab // total, slab), f32),
            pltpu.VMEM((total // 2, 4 * slab // total, slab), f32),
            pltpu.VMEM((2, slab, slab), f32),
            pltpu.VMEM((2, 2 * slab, slab), f32),
            pltpu.VMEM((2, slab, width), f32),
            pltpu.VMEM((2, total, TILE, width), f32),
            pltpu.VMEM((2, total, TILE, width), f32),
            pltpu.VMEM((total, 2, slab, width), f32),
            pltpu.VMEM((total, 2, slab, width), jnp.bfloat16),
            pltpu.VMEM((total, 2, slab, width), jnp.bfloat16),
            pltpu.VMEM((peers, total, pot.shape[1]), f32),
        ]
        + sems,
        compiler_params=pltpu.CompilerParams(collective_id=0, has_side_effects=True, vmem_limit_bytes=48 << 20),
    )(
        sets, proj, pot, strengths.reshape(1, -1), shifts.reshape(-1, 1),
        right[0], right[1], left[0], left[1],
    )
    return resp.transpose(2, 0, 1, 3), deriv.transpose(2, 1, 0, 3)


def solution(mesh):
    in_specs = (
        P("band", "kgrp", "pw", None),
        P("band", "kgrp", "pw", None),
        P("band", "kgrp", "pw", None),
        P("kgrp", None, "pw", None),
        P("pw", None),
        P(),
        P("band"),
    )
    out_specs = (P("band", "kgrp", "pw", None), P("band", "kgrp", "pw", None))
    def pick(*args):
        if local_plan_fits(args, mesh):
            return local_body(mesh, *args)
        return body(*args)

    return jax.shard_map(pick, mesh=mesh, in_specs=in_specs, out_specs=out_specs, check_vma=False)
```

```python
import functools
import math

import jax
import jax.numpy as jnp
import numpy as np
from jax import lax
from jax.experimental import pallas as pl
from jax.experimental.pallas import tpu as pltpu
from jax.sharding import PartitionSpec as P

ITERS = 2


precise = lax.Precision.HIGHEST
string_step = 0.05
kinetic_scale = 4.0


def margin(left_set, right_set):
    products = jnp.einsum("ixg,jyg->xyij", left_set, right_set, precision=precise)
    return jnp.stack([products[0, 0] + products[1, 1], products[0, 1] - products[1, 0]])


def combine(vectors, coeffs):
    table = jnp.stack([jnp.stack([coeffs[0], coeffs[1]]), jnp.stack([-coeffs[1], coeffs[0]])])
    return jnp.einsum("ixg,xyij->jyg", vectors, table, precision=precise)


def invert(matrix):
    real_part = matrix[0]
    imag_part = matrix[1]
    embedded = jnp.concatenate(
        [jnp.concatenate([real_part, -imag_part], 1), jnp.concatenate([imag_part, real_part], 1)], 0
    )
    normal = jnp.dot(embedded.T, embedded, precision=precise)
    lower_factor = jnp.linalg.cholesky(normal)
    middle = lax.linalg.triangular_solve(lower_factor, embedded.T, left_side=True, lower=True)
    inverse = lax.linalg.triangular_solve(
        lower_factor, middle, left_side=True, lower=True, transpose_a=True
    )
    count_rows = real_part.shape[0]
    return jnp.stack([inverse[:count_rows, :count_rows], inverse[count_rows:, :count_rows]])


def centred(index, length):
    shifted = (index + length // 2) % length - length // 2
    return shifted.astype(jnp.float32) / length


def dft_table(length, sign):
    index = jnp.arange(length, dtype=jnp.int32)
    phase = index[:, None] * index[None, :] % length
    angle = phase.astype(jnp.float32) * (2.0 * math.pi / length)
    cosine = jnp.cos(angle) / math.sqrt(length)
    sine = sign * jnp.sin(angle) / math.sqrt(length)
    return jnp.stack([jnp.stack([cosine, sine]), jnp.stack([-sine, cosine])])


def body(waves, forward, backward, projectors, potential, strengths, shifts):
    bands = waves.shape[0]
    rows = waves.shape[2]
    width = waves.shape[3]
    peers = lax.axis_size("pw")
    length = rows * peers
    points = float(length * width)
    cells = rows * width
    quarter = width // peers
    waves_flat = waves.reshape(bands, 2, cells)
    forward_flat = forward.reshape(bands, 2, cells)
    backward_flat = backward.reshape(bands, 2, cells)
    offset = lax.axis_index("band") * bands
    every_wave = lax.all_gather(waves_flat, "band", axis=0, tiled=True)
    forward_part = margin(every_wave, forward_flat) / points
    backward_part = margin(every_wave, backward_flat) / points
    forward_part, backward_part = lax.psum((forward_part, backward_part), "pw")
    forward_whole, backward_whole = (
        lax.all_gather(forward_part, "band", axis=2, tiled=True),
        lax.all_gather(backward_part, "band", axis=2, tiled=True),
    )
    forward_inverse = invert(forward_whole)
    backward_inverse = -invert(backward_whole)
    forward_cols = lax.dynamic_slice_in_dim(forward_inverse, offset, bands, 2)
    backward_cols = lax.dynamic_slice_in_dim(backward_inverse, offset, bands, 2)
    moved = combine(
        lax.all_gather(forward_flat, "band", axis=0, tiled=True), forward_cols
    ) + combine(lax.all_gather(backward_flat, "band", axis=0, tiled=True), backward_cols)
    derivative = (moved / (2.0 * string_step)).reshape(bands, 2, rows, width)
    first_index = lax.axis_index("pw") * rows + jnp.arange(rows, dtype=jnp.int32)
    second_index = jnp.arange(width, dtype=jnp.int32)
    first_freq = centred(first_index, length)
    second_freq = centred(second_index, width)
    kinetic = kinetic_scale * (
        first_freq[:, None] * first_freq[:, None] + second_freq[None, :] * second_freq[None, :]
    )
    diagonal = kinetic[None, None] + shifts[:, None, None, None]
    width_out = dft_table(width, 1.0)
    width_back = dft_table(width, -1.0)
    long_out = dft_table(length, 1.0).reshape(2, 2, peers, rows, length)
    long_back = dft_table(length, -1.0).reshape(2, 2, length, peers, rows)
    projector_flat = projectors.reshape(projectors.shape[0], 2, cells)
    residual = -derivative
    direction = residual
    solution = jnp.zeros_like(residual)
    norm_now = lax.psum(jnp.sum(residual * residual, axis=(1, 2, 3)), "pw")
    for turn in range(ITERS):
        sectioned = jnp.einsum("bxrj,xyjk->ykrb", direction, width_out, precision=precise).reshape(
            2, width, rows * bands
        )
        arrived = lax.all_to_all(sectioned, "pw", split_axis=1, concat_axis=2, tiled=True).reshape(
            2, quarter, peers, rows, bands
        )
        field = jnp.einsum("xqsrb,xysrk->yqbk", arrived, long_out, precision=precise)
        weighted = field * potential[None, :, None, :]
        leaving = jnp.einsum("xqbk,xyksr->yqsrb", weighted, long_back, precision=precise).reshape(
            2, quarter, peers * rows * bands
        )
        returned = lax.all_to_all(leaving, "pw", split_axis=2, concat_axis=1, tiled=True).reshape(
            2, width, rows, bands
        )
        smooth_part = jnp.einsum("xkrb,xykj->byrj", returned, width_back, precision=precise)
        coupling = margin(projector_flat, direction.reshape(bands, 2, cells)) / points
        own_energy = jnp.sum(diagonal * direction * direction, axis=(1, 2, 3)) + jnp.sum(
            weighted * field, axis=(0, 1, 3)
        )
        coupling, own_energy = lax.psum((coupling, own_energy), "pw")
        nonlocal_part = combine(projector_flat, coupling * strengths[None, :, None]).reshape(
            direction.shape
        )
        image = diagonal * direction + smooth_part + nonlocal_part
        curvature = own_energy + points * jnp.sum(
            strengths[None, :, None] * coupling * coupling, axis=(0, 1)
        )
        image, curvature = (image, curvature)
        alpha = (norm_now / curvature)[:, None, None, None]
        solution = solution + alpha * direction
        if turn + 1 < ITERS:
            residual = residual - alpha * image
            norm_next = lax.psum(jnp.sum(residual * residual, axis=(1, 2, 3)), "pw")
            direction = residual + (norm_next / norm_now)[:, None, None, None] * direction
            norm_now = norm_next
    return (solution, derivative)


MESH = pl.DeviceIdType.MESH
TILE = 8


def halves(x):
    high = x.astype(jnp.bfloat16)
    return high, (x - high.astype(jnp.float32)).astype(jnp.bfloat16)


def mul(a, b, turned=False):
    dims = (((1,), (1 if turned else 0,)), ((), ()))
    return lax.dot_general(a, b, dims, preferred_element_type=jnp.float32)


def mul3(a, b, turned=False):
    return mul(a[0], b[0], turned) + (mul(a[0], b[1], turned) + mul(a[1], b[0], turned))


def exact(a, b):
    return jnp.dot(a, b, precision=precise, preferred_element_type=jnp.float32)


def local_plan_fits(args, mesh):
    waves, projectors = args[0], args[3]
    peers, groups = mesh.shape["pw"], mesh.shape["band"]
    bands, rows, width = waves.shape[0], waves.shape[2], waves.shape[3]
    return (
        groups == 4
        and rows == groups
        and bands == TILE * peers
        and bands * groups == 128
        and projectors.shape[0] == 128
        and peers * rows == 16
        and width % 128 == 0
        and projectors.size * peers * 4 <= 8 << 20
    )


def local_kernel(
    peers, groups, sets, proj, pot, strengths, shifts, right_hi, right_lo, left_hi, left_lo,
    resp, deriv,
    got, marg, parts, whole, inv, both, made, field, answer, far, phi, plo, levels,
    s_send, s_recv, r_send, r_recv, g_send, g_recv, t_send, t_recv,
    p1_send, p1_recv, p2_send, p2_recv, p3_send, p3_recv, v_send, v_recv,
    x_send, x_recv, d_send, d_recv, o_send, o_recv,
):
    kgrp = lax.axis_index("kgrp")
    p = lax.axis_index("pw")
    b = lax.axis_index("band")
    core = lax.rem(b, 2)
    side = b // 2
    total = peers * groups
    mine = p * groups + b
    slot = p * 2 + side
    width = sets.shape[4]
    slab = groups * sets.shape[3]
    points = float(total * width)
    barrier = pltpu.get_barrier_semaphore()

    def flat(o):
        q = lax.rem(mine + o, total)
        return q // groups, lax.rem(q, groups)

    for o in range(1, total):
        q, c = flat(o)
        pl.semaphore_signal(barrier, inc=1, device_id=(kgrp, q, c), device_id_type=MESH)
    pl.semaphore_wait(barrier, total - 1)

    started = []

    def send(source, target, ssem, rsem, q, c):
        copy = pltpu.make_async_remote_copy(
            src_ref=source, dst_ref=target, send_sem=ssem, recv_sem=rsem,
            device_id=(kgrp, q, c), device_id_type=MESH,
        )
        copy.start()
        started.append(copy)
        return copy

    first = []
    for a in range(3):
        for o in range(1, groups):
            c = lax.rem(b + o, groups)
            k = a * groups + o
            first.append(send(sets.at[a, c], got.at[a, b], s_send.at[k], s_recv.at[k], p, c))
    pots, pass1, pass2, pass3 = [], [], [], []
    across = lax.rem(b + 2, groups)
    sibling = side * 2 + 1 - core
    for o in range(1, peers):
        q = lax.rem(p + o, peers)
        pots.append(send(pot, levels.at[p], v_send.at[o], v_recv.at[o], q, b))

    def spread_half(half):
        for o in range(1, peers):
            q = lax.rem(p + o, peers)
            k = half * peers + o
            pass1.append(send(proj.at[b, half], far.at[mine, half], p1_send.at[k], p1_recv.at[k], q, b))

    def cross_half(half):
        for o in range(1, peers):
            row = lax.rem(p + o, peers) * groups + b
            k = half * peers + o
            pass2.append(send(far.at[row, half], far.at[row, half], p2_send.at[k], p2_recv.at[k], p, across))

    def share_rows(j):
        for o in range(1, peers):
            row = lax.rem(p + o, peers) * groups + (b if j == 0 else across)
            k = 2 * o + j
            pass3.append(send(far.at[row], far.at[row], p3_send.at[k], p3_recv.at[k], p, sibling))

    spread_half(0)
    for a in range(3):
        got[a, b] = sets[a, b]
    levels[p] = pot[...]

    def set_of(a):
        return got[a, :, 0].reshape(slab, width), got[a, :, 1].reshape(slab, width)

    for copy in first[:3]:
        copy.wait_recv()
    wr, wi = set_of(0)
    lhs = halves(
        jnp.concatenate(
            [jnp.concatenate([wr, wi], 1), jnp.concatenate([-wi, wr], 1)], 0
        )
        * (1.0 / points)
    )
    for m in range(2):
        for copy in first[3 * m + 3 : 3 * m + 6]:
            copy.wait_recv()
        fr, fi = set_of(m + 1)
        part = mul3(lhs, halves(jnp.concatenate([fr, fi], 1)), True)
        marg[m] = part.reshape(marg.shape[1:])
    second = []
    for o in range(1, total):
        q, c = flat(o)
        second.append(
            send(marg.at[lax.rem(c, 2), q * 2 + c // 2], parts.at[mine], r_send.at[o], r_recv.at[o], q, c)
        )
    parts[mine] = marg[core, slot]
    def own_rows(r, carry):
        hi, lo = halves(proj[r])
        phi[p * groups + r] = hi
        plo[p * groups + r] = lo
        return carry

    lax.fori_loop(0, groups, own_rows, 0)
    for copy in second:
        copy.wait_recv()
    summed = parts[0]
    for k in range(1, total):
        summed = summed + parts[k]
    whole[slot] = summed
    third = []
    size = total // 2
    for o in range(1, size):
        s = lax.rem(slot + o, size)
        third.append(
            send(whole.at[slot], whole.at[slot], g_send.at[o], g_recv.at[o], s // 2, lax.rem(s, 2) * 2 + core)
        )
    for copy in pass1[: peers - 1]:
        copy.wait_recv()
    cross_half(0)
    spread_half(1)
    for copy in third:
        copy.wait_recv()
    stacked = whole[...].reshape(2 * slab, slab)
    ar, ai = stacked[:slab], stacked[slab:]
    turned = stacked.T
    inv[0] = exact(turned, stacked)
    inv[1] = exact(turned, jnp.concatenate([ai, -ar], 0))
    lane = lax.broadcasted_iota(jnp.int32, (slab, slab), 1)
    line = lax.broadcasted_iota(jnp.int32, (slab, slab), 0)
    lane1 = lax.broadcasted_iota(jnp.int32, (1, slab), 1)
    line1 = lax.broadcasted_iota(jnp.int32, (slab, 1), 0)

    def eliminate(k, carry):
        nr, ni = inv[0], inv[1]
        rr, ri = inv[0, pl.ds(k, 1), :], inv[1, pl.ds(k, 1), :]
        hit = lane == k
        cr = jnp.sum(jnp.where(hit, nr, 0.0), 1, keepdims=True)
        ci = jnp.sum(jnp.where(hit, ni, 0.0), 1, keepdims=True)
        own = lane1 == k
        scale = 1.0 / jnp.sum(jnp.where(own, rr, 0.0), 1, keepdims=True)
        sr = jnp.where(own, 1.0, rr) * scale
        si = jnp.where(own, 0.0, ri) * scale
        cr = jnp.where(line1 == k, -1.0, cr)
        ci = jnp.where(line1 == k, 0.0, ci)
        gone = jnp.logical_or(hit, line == k)
        inv[0] = jnp.where(gone, 0.0, nr) - (cr * sr - ci * si)
        inv[1] = jnp.where(gone, 0.0, ni) - (cr * si + ci * sr)
        return carry

    lax.fori_loop(0, slab * 5 // 8, eliminate, 0)
    for copy in pass1[peers - 1 :]:
        copy.wait_recv()
    cross_half(1)
    share_rows(0)
    lax.fori_loop(slab * 5 // 8, slab, eliminate, 0)
    kr, ki = inv[0], inv[1]
    mixed = exact(
        jnp.concatenate([jnp.concatenate([ar, -ai], 1), jnp.concatenate([-ai, -ar], 1)], 0),
        jnp.concatenate([kr, ki], 0),
    )
    sign = (1 - 2 * core).astype(jnp.float32) / (2.0 * string_step)
    both[core] = mixed * sign
    swap = send(both.at[core], both.at[core], t_send, t_recv, p, sibling)
    for copy in pass2:
        copy.wait_recv()
    share_rows(1)
    fr, fi = set_of(1)
    br, bi = set_of(2)
    rhs = halves(jnp.concatenate([fr, fi, br, bi], 0))
    swap.wait_recv()
    f, g = both[0], both[1]
    tfr, tfi, tbr, tbi = f[:slab], f[slab:], g[:slab], g[slab:]
    table = halves(
        jnp.concatenate(
            [
                jnp.concatenate([tfr, -tfi, tbr, -tbi], 1),
                jnp.concatenate([tfi, tfr, tbi, tbr], 1),
            ],
            0,
        )
    )
    made[...] = mul3(table, rhs).reshape(made.shape)
    fields, outs = [], []
    for o in range(1, total):
        q, c = flat(o)
        rows = pl.ds(pl.multiple_of((c * peers + q) * TILE, TILE), TILE)
        fields.append(send(made.at[:, rows], field.at[:, mine], x_send.at[o], x_recv.at[o], q, c))
    span = slab // groups
    for o in range(1, groups):
        c = lax.rem(b + o, groups)
        rows = pl.ds(pl.multiple_of(c * span, TILE), span)
        outs.append(send(made.at[:, rows], deriv.at[b], d_send.at[o], d_recv.at[o], p, c))
    field[:, mine] = made[:, pl.ds(pl.multiple_of((b * peers + p) * TILE, TILE), TILE)]
    deriv[b] = made[:, pl.ds(pl.multiple_of(b * span, TILE), span)]
    for copy in pass3:
        copy.wait_recv()

    def far_rows(t, carry):
        row = lax.rem(p * groups + groups + t, total)
        hi, lo = halves(far[row])
        phi[row] = hi
        plo[row] = lo
        return carry

    lax.fori_loop(0, total - groups, far_rows, 0)
    for copy in pots:
        copy.wait_recv()
    share = width // peers
    level = jnp.concatenate([levels[k][:, :share] for k in range(peers)], 1)
    level = jnp.broadcast_to(level[:, None, :], (total, TILE, width)).reshape(total * TILE, width)
    iu = lax.broadcasted_iota(jnp.int32, (total, TILE, width), 0)
    iw = lax.broadcasted_iota(jnp.int32, (total, TILE, width), 2)
    fu = jnp.where(iu < total // 2, iu, iu - total).astype(jnp.float32) / total
    fw = jnp.where(iw < width // 2, iw, iw - width).astype(jnp.float32) / width
    shift = shifts[pl.ds(pl.multiple_of(p * TILE, TILE), TILE), :]
    diagonal = kinetic_scale * (fu * fu + fw * fw) + shift[None]
    diagonal = diagonal.reshape(total * TILE, width)
    for copy in fields:
        copy.wait_recv()

    def transform(xr, xi):
        y = mul3(halves(jnp.concatenate([xr, xi], 1)), (right_hi[...], right_lo[...]))
        y = jnp.concatenate([y[:, :width], y[:, width:]], 0)
        z = mul3((left_hi[...], left_lo[...]), halves(y))
        return z[: total * TILE], z[total * TILE :]

    def energy(dr, di):
        yr, yi = transform(dr, di)
        coupling = project(dr, di)
        local = summed_over(diagonal * (dr * dr + di * di) + level * (yr * yr + yi * yi))
        weight = jnp.sum(coupling * coupling * strengths[...], 1, keepdims=True) * points
        return local + weight[:TILE] + weight[TILE:]

    def project(dr, di):
        accr = jnp.zeros((2 * TILE, slab), jnp.float32)
        acci = jnp.zeros((2 * TILE, slab), jnp.float32)
        for i in range(total):
            at = slice(i * TILE, i * TILE + TILE)
            hi, lo = halves(jnp.concatenate([dr[at], di[at]], 0))
            accr = accr + mul3((hi, lo), (phi[i, 0], plo[i, 0]), True)
            acci = acci + mul3((hi, lo), (phi[i, 1], plo[i, 1]), True)
        return jnp.concatenate(
            [accr[:TILE] + acci[TILE:], accr[TILE:] - acci[:TILE]], 0
        ) * (1.0 / points)

    def operate(dr, di):
        yr, yi = transform(dr, di)
        zr, zi = transform(yr * level, -(yi * level))
        c2 = halves(project(dr, di) * strengths[...])
        outr, outi = [], []
        for i in range(total):
            ur = mul3(c2, (phi[i, 0], plo[i, 0]))
            ui = mul3(c2, (phi[i, 1], plo[i, 1]))
            outr.append(ur[:TILE] - ui[TILE:])
            outi.append(ui[:TILE] + ur[TILE:])
        return (
            diagonal * dr + zr + jnp.concatenate(outr, 0),
            diagonal * di - zi + jnp.concatenate(outi, 0),
        )

    def summed_over(x):
        x = x.reshape(total, TILE, width)
        return jnp.sum(jnp.sum(x, 0), 1, keepdims=True)

    def spread(x):
        return jnp.broadcast_to(x[None], (total, TILE, width)).reshape(total * TILE, width)

    rr = -field[0].reshape(total * TILE, width)
    ri = -field[1].reshape(total * TILE, width)
    dr, di = rr, ri
    norm_now = summed_over(rr * rr + ri * ri)
    solr, soli = jnp.zeros_like(dr), jnp.zeros_like(di)
    for turn in range(ITERS):
        if turn + 1 < ITERS:
            imr, imi = operate(dr, di)
            curvature = summed_over(dr * imr + di * imi)
        else:
            curvature = energy(dr, di)
        alpha = spread(norm_now / curvature)
        solr, soli = solr + alpha * dr, soli + alpha * di
        if turn + 1 < ITERS:
            rr, ri = rr - alpha * imr, ri - alpha * imi
            norm_next = summed_over(rr * rr + ri * ri)
            beta = spread(norm_next / norm_now)
            dr, di = rr + beta * dr, ri + beta * di
            norm_now = norm_next
    answer[0] = solr.reshape(total, TILE, width)
    answer[1] = soli.reshape(total, TILE, width)
    here = pl.ds(pl.multiple_of(p * TILE, TILE), TILE)
    for o in range(1, peers):
        q = lax.rem(p + o, peers)
        outs.append(
            send(answer.at[:, pl.ds(q * groups, groups)], resp.at[:, :, here], o_send.at[o], o_recv.at[o], q, b)
        )
    resp[:, :, here] = answer[:, pl.ds(p * groups, groups)]
    for copy in outs:
        copy.wait_recv()
    for copy in started:
        copy.wait_send()


def tables(length, repeat):
    index = np.arange(length)
    angle = (index[:, None] * index[None, :] % length) * (2.0 * math.pi / length)
    eye = np.eye(repeat)
    cosine = np.kron(np.cos(angle) / math.sqrt(length), eye)
    sine = np.kron(np.sin(angle) / math.sqrt(length), eye)
    return cosine.astype(np.float32), sine.astype(np.float32)


def split_table(table):
    return halves(jnp.asarray(table))


def local_body(mesh, waves, forward, backward, projectors, potential, strengths, shifts):
    peers, groups = mesh.shape["pw"], mesh.shape["band"]
    bands, _, rows, width = waves.shape
    slab, total = bands * groups, peers * rows
    sets = jnp.stack([waves, forward, backward]).transpose(0, 3, 2, 1, 4)
    proj = projectors.transpose(2, 1, 0, 3)
    pot = jnp.pad(potential.T, ((0, 0), (0, 128 - potential.shape[0] % 128)))
    c, s = tables(width, 1)
    right = split_table(np.block([[c, s], [-s, c]]))
    c, s = tables(total, TILE)
    left = split_table(np.block([[c, -s], [s, c]]))
    f32 = jnp.float32
    dma = pltpu.SemaphoreType.DMA
    vmem = pl.BlockSpec(memory_space=pltpu.VMEM)
    sems = []
    for count in (3 * groups, total, total // 2):
        sems += [dma((count,)), dma((count,))]
    sems += [dma, dma]
    for count in (2 * peers, 2 * peers, 2 * peers, peers, total, groups, peers):
        sems += [dma((count,)), dma((count,))]
    resp, deriv = pl.pallas_call(
        functools.partial(local_kernel, peers, groups),
        out_shape=(
            jax.ShapeDtypeStruct((2, rows, bands, width), f32),
            jax.ShapeDtypeStruct((rows, 2, bands, width), f32),
        ),
        in_specs=[vmem] * 9,
        out_specs=(vmem, vmem),
        scratch_shapes=[
            pltpu.VMEM((3, groups, 2, bands, width), f32),
            pltpu.VMEM((2, total // 2, 4 * slab // total, slab), f32),
            pltpu.VMEM((total, 4 * slab // total, slab), f32),
            pltpu.VMEM((total // 2, 4 * slab // total, slab), f32),
            pltpu.VMEM((2, slab, slab), f32),
            pltpu.VMEM((2, 2 * slab, slab), f32),
            pltpu.VMEM((2, slab, width), f32),
            pltpu.VMEM((2, total, TILE, width), f32),
            pltpu.VMEM((2, total, TILE, width), f32),
            pltpu.VMEM((total, 2, slab, width), f32),
            pltpu.VMEM((total, 2, slab, width), jnp.bfloat16),
            pltpu.VMEM((total, 2, slab, width), jnp.bfloat16),
            pltpu.VMEM((peers, total, pot.shape[1]), f32),
        ]
        + sems,
        compiler_params=pltpu.CompilerParams(collective_id=0, has_side_effects=True, vmem_limit_bytes=48 << 20),
    )(
        sets, proj, pot, strengths.reshape(1, -1), shifts.reshape(-1, 1),
        right[0], right[1], left[0], left[1],
    )
    return resp.transpose(2, 0, 1, 3), deriv.transpose(2, 1, 0, 3)


def solution(mesh):
    in_specs = (
        P("band", "kgrp", "pw", None),
        P("band", "kgrp", "pw", None),
        P("band", "kgrp", "pw", None),
        P("kgrp", None, "pw", None),
        P("pw", None),
        P(),
        P("band"),
    )
    out_specs = (P("band", "kgrp", "pw", None), P("band", "kgrp", "pw", None))
    def pick(*args):
        if local_plan_fits(args, mesh):
            return local_body(mesh, *args)
        return body(*args)

    return jax.shard_map(pick, mesh=mesh, in_specs=in_specs, out_specs=out_specs, check_vma=False)
```

```python
import functools
import math

import jax
import jax.numpy as jnp
import numpy as np
from jax import lax
from jax.experimental import pallas as pl
from jax.experimental.pallas import tpu as pltpu
from jax.sharding import PartitionSpec as P

ITERS = 2


precise = lax.Precision.HIGHEST
string_step = 0.05
kinetic_scale = 4.0


def margin(left_set, right_set):
    products = jnp.einsum("ixg,jyg->xyij", left_set, right_set, precision=precise)
    return jnp.stack([products[0, 0] + products[1, 1], products[0, 1] - products[1, 0]])


def combine(vectors, coeffs):
    table = jnp.stack([jnp.stack([coeffs[0], coeffs[1]]), jnp.stack([-coeffs[1], coeffs[0]])])
    return jnp.einsum("ixg,xyij->jyg", vectors, table, precision=precise)


def invert(matrix):
    real_part = matrix[0]
    imag_part = matrix[1]
    embedded = jnp.concatenate(
        [jnp.concatenate([real_part, -imag_part], 1), jnp.concatenate([imag_part, real_part], 1)], 0
    )
    normal = jnp.dot(embedded.T, embedded, precision=precise)
    lower_factor = jnp.linalg.cholesky(normal)
    middle = lax.linalg.triangular_solve(lower_factor, embedded.T, left_side=True, lower=True)
    inverse = lax.linalg.triangular_solve(
        lower_factor, middle, left_side=True, lower=True, transpose_a=True
    )
    count_rows = real_part.shape[0]
    return jnp.stack([inverse[:count_rows, :count_rows], inverse[count_rows:, :count_rows]])


def centred(index, length):
    shifted = (index + length // 2) % length - length // 2
    return shifted.astype(jnp.float32) / length


def dft_table(length, sign):
    index = jnp.arange(length, dtype=jnp.int32)
    phase = index[:, None] * index[None, :] % length
    angle = phase.astype(jnp.float32) * (2.0 * math.pi / length)
    cosine = jnp.cos(angle) / math.sqrt(length)
    sine = sign * jnp.sin(angle) / math.sqrt(length)
    return jnp.stack([jnp.stack([cosine, sine]), jnp.stack([-sine, cosine])])


def body(waves, forward, backward, projectors, potential, strengths, shifts):
    bands = waves.shape[0]
    rows = waves.shape[2]
    width = waves.shape[3]
    peers = lax.axis_size("pw")
    length = rows * peers
    points = float(length * width)
    cells = rows * width
    quarter = width // peers
    waves_flat = waves.reshape(bands, 2, cells)
    forward_flat = forward.reshape(bands, 2, cells)
    backward_flat = backward.reshape(bands, 2, cells)
    offset = lax.axis_index("band") * bands
    every_wave = lax.all_gather(waves_flat, "band", axis=0, tiled=True)
    forward_part = margin(every_wave, forward_flat) / points
    backward_part = margin(every_wave, backward_flat) / points
    forward_part, backward_part = lax.psum((forward_part, backward_part), "pw")
    forward_whole, backward_whole = (
        lax.all_gather(forward_part, "band", axis=2, tiled=True),
        lax.all_gather(backward_part, "band", axis=2, tiled=True),
    )
    forward_inverse = invert(forward_whole)
    backward_inverse = -invert(backward_whole)
    forward_cols = lax.dynamic_slice_in_dim(forward_inverse, offset, bands, 2)
    backward_cols = lax.dynamic_slice_in_dim(backward_inverse, offset, bands, 2)
    moved = combine(
        lax.all_gather(forward_flat, "band", axis=0, tiled=True), forward_cols
    ) + combine(lax.all_gather(backward_flat, "band", axis=0, tiled=True), backward_cols)
    derivative = (moved / (2.0 * string_step)).reshape(bands, 2, rows, width)
    first_index = lax.axis_index("pw") * rows + jnp.arange(rows, dtype=jnp.int32)
    second_index = jnp.arange(width, dtype=jnp.int32)
    first_freq = centred(first_index, length)
    second_freq = centred(second_index, width)
    kinetic = kinetic_scale * (
        first_freq[:, None] * first_freq[:, None] + second_freq[None, :] * second_freq[None, :]
    )
    diagonal = kinetic[None, None] + shifts[:, None, None, None]
    width_out = dft_table(width, 1.0)
    width_back = dft_table(width, -1.0)
    long_out = dft_table(length, 1.0).reshape(2, 2, peers, rows, length)
    long_back = dft_table(length, -1.0).reshape(2, 2, length, peers, rows)
    projector_flat = projectors.reshape(projectors.shape[0], 2, cells)
    residual = -derivative
    direction = residual
    solution = jnp.zeros_like(residual)
    norm_now = lax.psum(jnp.sum(residual * residual, axis=(1, 2, 3)), "pw")
    for turn in range(ITERS):
        sectioned = jnp.einsum("bxrj,xyjk->ykrb", direction, width_out, precision=precise).reshape(
            2, width, rows * bands
        )
        arrived = lax.all_to_all(sectioned, "pw", split_axis=1, concat_axis=2, tiled=True).reshape(
            2, quarter, peers, rows, bands
        )
        field = jnp.einsum("xqsrb,xysrk->yqbk", arrived, long_out, precision=precise)
        weighted = field * potential[None, :, None, :]
        leaving = jnp.einsum("xqbk,xyksr->yqsrb", weighted, long_back, precision=precise).reshape(
            2, quarter, peers * rows * bands
        )
        returned = lax.all_to_all(leaving, "pw", split_axis=2, concat_axis=1, tiled=True).reshape(
            2, width, rows, bands
        )
        smooth_part = jnp.einsum("xkrb,xykj->byrj", returned, width_back, precision=precise)
        coupling = margin(projector_flat, direction.reshape(bands, 2, cells)) / points
        own_energy = jnp.sum(diagonal * direction * direction, axis=(1, 2, 3)) + jnp.sum(
            weighted * field, axis=(0, 1, 3)
        )
        coupling, own_energy = lax.psum((coupling, own_energy), "pw")
        nonlocal_part = combine(projector_flat, coupling * strengths[None, :, None]).reshape(
            direction.shape
        )
        image = diagonal * direction + smooth_part + nonlocal_part
        curvature = own_energy + points * jnp.sum(
            strengths[None, :, None] * coupling * coupling, axis=(0, 1)
        )
        image, curvature = (image, curvature)
        alpha = (norm_now / curvature)[:, None, None, None]
        solution = solution + alpha * direction
        if turn + 1 < ITERS:
            residual = residual - alpha * image
            norm_next = lax.psum(jnp.sum(residual * residual, axis=(1, 2, 3)), "pw")
            direction = residual + (norm_next / norm_now)[:, None, None, None] * direction
            norm_now = norm_next
    return (solution, derivative)


MESH = pl.DeviceIdType.MESH
TILE = 8


def halves(x):
    high = x.astype(jnp.bfloat16)
    return high, (x - high.astype(jnp.float32)).astype(jnp.bfloat16)


def mul(a, b, turned=False):
    dims = (((1,), (1 if turned else 0,)), ((), ()))
    return lax.dot_general(a, b, dims, preferred_element_type=jnp.float32)


def mul3(a, b, turned=False):
    return mul(a[0], b[0], turned) + (mul(a[0], b[1], turned) + mul(a[1], b[0], turned))


def exact(a, b):
    return jnp.dot(a, b, precision=precise, preferred_element_type=jnp.float32)


def local_plan_fits(args, mesh):
    waves, projectors = args[0], args[3]
    peers, groups = mesh.shape["pw"], mesh.shape["band"]
    bands, rows, width = waves.shape[0], waves.shape[2], waves.shape[3]
    return (
        groups == 4
        and rows == groups
        and bands == TILE * peers
        and bands * groups == 128
        and projectors.shape[0] == 128
        and peers * rows == 16
        and width % 128 == 0
        and projectors.size * peers * 4 <= 8 << 20
    )


def local_kernel(
    peers, groups, waves, ahead, behind, proj, pot, strengths, shifts, right_hi, right_lo, left_hi, left_lo,
    resp, deriv,
    got, marg, pair, merged, parts, whole, inv, both, made, field, answer, far, phi, plo, levels,
    s_send, s_recv, m_send, m_recv, r_send, r_recv, g_send, g_recv, t_send, t_recv,
    p1_send, p1_recv, p2_send, p2_recv, p3_send, p3_recv, v_send, v_recv,
    x_send, x_recv, d_send, d_recv, o_send, o_recv,
):
    sets = (waves, ahead, behind)
    kgrp = lax.axis_index("kgrp")
    p = lax.axis_index("pw")
    b = lax.axis_index("band")
    core = lax.rem(b, 2)
    side = b // 2
    total = peers * groups
    mine = p * groups + b
    slot = p * 2 + side
    width = waves.shape[3]
    slab = groups * waves.shape[2]
    points = float(total * width)
    barrier = pltpu.get_barrier_semaphore()

    def flat(o):
        q = lax.rem(mine + o, total)
        return q // groups, lax.rem(q, groups)

    for o in range(1, total):
        q, c = flat(o)
        pl.semaphore_signal(barrier, inc=1, device_id=(kgrp, q, c), device_id_type=MESH)
    pl.semaphore_wait(barrier, total - 1)

    started = []

    def send(source, target, ssem, rsem, q, c):
        copy = pltpu.make_async_remote_copy(
            src_ref=source, dst_ref=target, send_sem=ssem, recv_sem=rsem,
            device_id=(kgrp, q, c), device_id_type=MESH,
        )
        copy.start()
        started.append(copy)
        return copy

    first = []
    for a in range(3):
        for o in range(1, groups):
            c = lax.rem(b + o, groups)
            k = a * groups + o
            first.append(send(sets[a].at[c], got.at[a, b], s_send.at[k], s_recv.at[k], p, c))
    pots, pass1, pass2, pass3 = [], [], [], []
    across = lax.rem(b + 2, groups)
    sibling = side * 2 + 1 - core
    for o in range(1, peers):
        q = lax.rem(p + o, peers)
        pots.append(send(pot, levels.at[p], v_send.at[o], v_recv.at[o], q, b))

    def spread_half(half):
        for o in range(1, peers):
            q = lax.rem(p + o, peers)
            k = half * peers + o
            pass1.append(send(proj.at[b, half], far.at[mine, half], p1_send.at[k], p1_recv.at[k], q, b))

    def cross_half(half):
        for o in range(1, peers):
            row = lax.rem(p + o, peers) * groups + b
            k = half * peers + o
            pass2.append(send(far.at[row, half], far.at[row, half], p2_send.at[k], p2_recv.at[k], p, across))

    def share_rows(j):
        for o in range(1, peers):
            row = lax.rem(p + o, peers) * groups + (b if j == 0 else across)
            k = 2 * o + j
            pass3.append(send(far.at[row], far.at[row], p3_send.at[k], p3_recv.at[k], p, sibling))

    spread_half(0)
    for a in range(3):
        got[a, b] = sets[a][b]
    levels[p] = pot[...]

    def set_of(a):
        return got[a, :, 0].reshape(slab, width), got[a, :, 1].reshape(slab, width)

    for copy in first[:3]:
        copy.wait_recv()
    wr, wi = set_of(0)
    lhs = halves(
        jnp.concatenate(
            [jnp.concatenate([wr, wi], 1), jnp.concatenate([-wi, wr], 1)], 0
        )
        * (1.0 / points)
    )
    for m in range(2):
        for copy in first[3 * m + 3 : 3 * m + 6]:
            copy.wait_recv()
        fr, fi = set_of(m + 1)
        part = mul3(lhs, halves(jnp.concatenate([fr, fi], 1)), True)
        marg[m] = part.reshape(marg.shape[1:])
    joined = send(marg.at[1 - core], pair, m_send, m_recv, p, sibling)
    joined.wait_recv()
    merged[...] = marg[core] + pair[...]
    second = []
    size = total // 2
    for o in range(1, size):
        s = lax.rem(slot + o, size)
        second.append(
            send(merged.at[s], parts.at[slot], r_send.at[o], r_recv.at[o], s // 2, lax.rem(s, 2) * 2 + core)
        )
    parts[slot] = merged[slot]

    def own_rows(r, carry):
        hi, lo = halves(proj[r])
        phi[p * groups + r] = hi
        plo[p * groups + r] = lo
        return carry

    lax.fori_loop(0, groups, own_rows, 0)
    for copy in second:
        copy.wait_recv()
    summed = parts[0]
    for k in range(1, size):
        summed = summed + parts[k]
    whole[slot] = summed
    third = []
    for o in range(1, size):
        s = lax.rem(slot + o, size)
        third.append(
            send(whole.at[slot], whole.at[slot], g_send.at[o], g_recv.at[o], s // 2, lax.rem(s, 2) * 2 + core)
        )
    for copy in pass1[: peers - 1]:
        copy.wait_recv()
    cross_half(0)
    spread_half(1)
    for copy in third:
        copy.wait_recv()
    stacked = whole[...].reshape(2 * slab, slab)
    ar, ai = stacked[:slab], stacked[slab:]
    turned = stacked.T
    inv[0] = exact(turned, stacked)
    inv[1] = exact(turned, jnp.concatenate([ai, -ar], 0))
    lane = lax.broadcasted_iota(jnp.int32, (slab, slab), 1)
    line = lax.broadcasted_iota(jnp.int32, (slab, slab), 0)
    lane1 = lax.broadcasted_iota(jnp.int32, (1, slab), 1)
    line1 = lax.broadcasted_iota(jnp.int32, (slab, 1), 0)

    def eliminate(k, carry):
        nr, ni = inv[0], inv[1]
        rr, ri = inv[0, pl.ds(k, 1), :], inv[1, pl.ds(k, 1), :]
        hit = lane == k
        cr = jnp.sum(jnp.where(hit, nr, 0.0), 1, keepdims=True)
        ci = jnp.sum(jnp.where(hit, ni, 0.0), 1, keepdims=True)
        own = lane1 == k
        scale = 1.0 / jnp.sum(jnp.where(own, rr, 0.0), 1, keepdims=True)
        sr = jnp.where(own, 1.0, rr) * scale
        si = jnp.where(own, 0.0, ri) * scale
        cr = jnp.where(line1 == k, -1.0, cr)
        ci = jnp.where(line1 == k, 0.0, ci)
        gone = jnp.logical_or(hit, line == k)
        inv[0] = jnp.where(gone, 0.0, nr) - (cr * sr - ci * si)
        inv[1] = jnp.where(gone, 0.0, ni) - (cr * si + ci * sr)
        return carry

    lax.fori_loop(0, slab * 5 // 8, eliminate, 0)
    for copy in pass1[peers - 1 :]:
        copy.wait_recv()
    cross_half(1)
    share_rows(0)
    lax.fori_loop(slab * 5 // 8, slab, eliminate, 0)
    kr, ki = inv[0], inv[1]
    mixed = exact(
        jnp.concatenate([jnp.concatenate([ar, -ai], 1), jnp.concatenate([-ai, -ar], 1)], 0),
        jnp.concatenate([kr, ki], 0),
    )
    sign = (1 - 2 * core).astype(jnp.float32) / (2.0 * string_step)
    both[core] = mixed * sign
    swap = send(both.at[core], both.at[core], t_send, t_recv, p, sibling)
    for copy in pass2:
        copy.wait_recv()
    share_rows(1)
    fr, fi = set_of(1)
    br, bi = set_of(2)
    rhs = halves(jnp.concatenate([fr, fi, br, bi], 0))
    swap.wait_recv()
    f, g = both[0], both[1]
    tfr, tfi, tbr, tbi = f[:slab], f[slab:], g[:slab], g[slab:]
    table = halves(
        jnp.concatenate(
            [
                jnp.concatenate([tfr, -tfi, tbr, -tbi], 1),
                jnp.concatenate([tfi, tfr, tbi, tbr], 1),
            ],
            0,
        )
    )
    made[...] = mul3(table, rhs).reshape(made.shape)
    fields, outs = [], []
    for o in range(1, total):
        q, c = flat(o)
        rows = pl.ds(pl.multiple_of((c * peers + q) * TILE, TILE), TILE)
        fields.append(send(made.at[:, rows], field.at[:, mine], x_send.at[o], x_recv.at[o], q, c))
    span = slab // groups
    for o in range(1, groups):
        c = lax.rem(b + o, groups)
        rows = pl.ds(pl.multiple_of(c * span, TILE), span)
        outs.append(send(made.at[:, rows], deriv.at[b], d_send.at[o], d_recv.at[o], p, c))
    field[:, mine] = made[:, pl.ds(pl.multiple_of((b * peers + p) * TILE, TILE), TILE)]
    deriv[b] = made[:, pl.ds(pl.multiple_of(b * span, TILE), span)]
    for copy in pass3:
        copy.wait_recv()

    def far_rows(t, carry):
        row = lax.rem(p * groups + groups + t, total)
        hi, lo = halves(far[row])
        phi[row] = hi
        plo[row] = lo
        return carry

    lax.fori_loop(0, total - groups, far_rows, 0)
    for copy in pots:
        copy.wait_recv()
    share = width // peers
    level = jnp.concatenate([levels[k][:, :share] for k in range(peers)], 1)
    level = jnp.broadcast_to(level[:, None, :], (total, TILE, width)).reshape(total * TILE, width)
    iu = lax.broadcasted_iota(jnp.int32, (total, TILE, width), 0)
    iw = lax.broadcasted_iota(jnp.int32, (total, TILE, width), 2)
    fu = jnp.where(iu < total // 2, iu, iu - total).astype(jnp.float32) / total
    fw = jnp.where(iw < width // 2, iw, iw - width).astype(jnp.float32) / width
    shift = shifts[pl.ds(pl.multiple_of(p * TILE, TILE), TILE), :]
    diagonal = kinetic_scale * (fu * fu + fw * fw) + shift[None]
    diagonal = diagonal.reshape(total * TILE, width)
    for copy in fields:
        copy.wait_recv()

    def transform(xr, xi):
        y = mul3(halves(jnp.concatenate([xr, xi], 1)), (right_hi[...], right_lo[...]))
        y = jnp.concatenate([y[:, :width], y[:, width:]], 0)
        z = mul3((left_hi[...], left_lo[...]), halves(y))
        return z[: total * TILE], z[total * TILE :]

    def energy(dr, di):
        yr, yi = transform(dr, di)
        coupling = project(dr, di)
        local = summed_over(diagonal * (dr * dr + di * di) + level * (yr * yr + yi * yi))
        weight = jnp.sum(coupling * coupling * strengths[...], 1, keepdims=True) * points
        return local + weight[:TILE] + weight[TILE:]

    def project(dr, di):
        accr = jnp.zeros((2 * TILE, slab), jnp.float32)
        acci = jnp.zeros((2 * TILE, slab), jnp.float32)
        for i in range(total):
            at = slice(i * TILE, i * TILE + TILE)
            hi, lo = halves(jnp.concatenate([dr[at], di[at]], 0))
            accr = accr + mul3((hi, lo), (phi[i, 0], plo[i, 0]), True)
            acci = acci + mul3((hi, lo), (phi[i, 1], plo[i, 1]), True)
        return jnp.concatenate(
            [accr[:TILE] + acci[TILE:], accr[TILE:] - acci[:TILE]], 0
        ) * (1.0 / points)

    def operate(dr, di):
        yr, yi = transform(dr, di)
        zr, zi = transform(yr * level, -(yi * level))
        c2 = halves(project(dr, di) * strengths[...])
        outr, outi = [], []
        for i in range(total):
            ur = mul3(c2, (phi[i, 0], plo[i, 0]))
            ui = mul3(c2, (phi[i, 1], plo[i, 1]))
            outr.append(ur[:TILE] - ui[TILE:])
            outi.append(ui[:TILE] + ur[TILE:])
        return (
            diagonal * dr + zr + jnp.concatenate(outr, 0),
            diagonal * di - zi + jnp.concatenate(outi, 0),
        )

    def summed_over(x):
        x = x.reshape(total, TILE, width)
        return jnp.sum(jnp.sum(x, 0), 1, keepdims=True)

    def spread(x):
        return jnp.broadcast_to(x[None], (total, TILE, width)).reshape(total * TILE, width)

    rr = -field[0].reshape(total * TILE, width)
    ri = -field[1].reshape(total * TILE, width)
    dr, di = rr, ri
    norm_now = summed_over(rr * rr + ri * ri)
    solr, soli = jnp.zeros_like(dr), jnp.zeros_like(di)
    for turn in range(ITERS):
        if turn + 1 < ITERS:
            imr, imi = operate(dr, di)
            curvature = summed_over(dr * imr + di * imi)
        else:
            curvature = energy(dr, di)
        alpha = spread(norm_now / curvature)
        solr, soli = solr + alpha * dr, soli + alpha * di
        if turn + 1 < ITERS:
            rr, ri = rr - alpha * imr, ri - alpha * imi
            norm_next = summed_over(rr * rr + ri * ri)
            beta = spread(norm_next / norm_now)
            dr, di = rr + beta * dr, ri + beta * di
            norm_now = norm_next
    answer[0] = solr.reshape(total, TILE, width)
    answer[1] = soli.reshape(total, TILE, width)
    here = pl.ds(pl.multiple_of(p * TILE, TILE), TILE)
    for o in range(1, peers):
        q = lax.rem(p + o, peers)
        outs.append(
            send(answer.at[:, pl.ds(q * groups, groups)], resp.at[:, :, here], o_send.at[o], o_recv.at[o], q, b)
        )
    resp[:, :, here] = answer[:, pl.ds(p * groups, groups)]
    for copy in outs:
        copy.wait_recv()
    for copy in started:
        copy.wait_send()


def tables(length, repeat):
    index = np.arange(length)
    angle = (index[:, None] * index[None, :] % length) * (2.0 * math.pi / length)
    eye = np.eye(repeat)
    cosine = np.kron(np.cos(angle) / math.sqrt(length), eye)
    sine = np.kron(np.sin(angle) / math.sqrt(length), eye)
    return cosine.astype(np.float32), sine.astype(np.float32)


def split_table(table):
    return halves(jnp.asarray(table))


def local_body(mesh, waves, forward, backward, projectors, potential, strengths, shifts):
    peers, groups = mesh.shape["pw"], mesh.shape["band"]
    bands, _, rows, width = waves.shape
    slab, total = bands * groups, peers * rows
    sets = [x.transpose(2, 1, 0, 3) for x in (waves, forward, backward)]
    proj = projectors.transpose(2, 1, 0, 3)
    pot = jnp.pad(potential.T, ((0, 0), (0, 128 - potential.shape[0] % 128)))
    c, s = tables(width, 1)
    right = split_table(np.block([[c, s], [-s, c]]))
    c, s = tables(total, TILE)
    left = split_table(np.block([[c, -s], [s, c]]))
    f32 = jnp.float32
    dma = pltpu.SemaphoreType.DMA
    vmem = pl.BlockSpec(memory_space=pltpu.VMEM)
    sems = []
    for count in ((3 * groups,), (), (total // 2,), (total // 2,), ()):
        sems += [dma(count) if count else dma, dma(count) if count else dma]
    for count in (2 * peers, 2 * peers, 2 * peers, peers, total, groups, peers):
        sems += [dma((count,)), dma((count,))]
    resp, deriv = pl.pallas_call(
        functools.partial(local_kernel, peers, groups),
        out_shape=(
            jax.ShapeDtypeStruct((2, rows, bands, width), f32),
            jax.ShapeDtypeStruct((rows, 2, bands, width), f32),
        ),
        in_specs=[vmem] * 11,
        out_specs=(vmem, vmem),
        scratch_shapes=[
            pltpu.VMEM((3, groups, 2, bands, width), f32),
            pltpu.VMEM((2, total // 2, 4 * slab // total, slab), f32),
            pltpu.VMEM((total // 2, 4 * slab // total, slab), f32),
            pltpu.VMEM((total // 2, 4 * slab // total, slab), f32),
            pltpu.VMEM((total // 2, 4 * slab // total, slab), f32),
            pltpu.VMEM((total // 2, 4 * slab // total, slab), f32),
            pltpu.VMEM((2, slab, slab), f32),
            pltpu.VMEM((2, 2 * slab, slab), f32),
            pltpu.VMEM((2, slab, width), f32),
            pltpu.VMEM((2, total, TILE, width), f32),
            pltpu.VMEM((2, total, TILE, width), f32),
            pltpu.VMEM((total, 2, slab, width), f32),
            pltpu.VMEM((total, 2, slab, width), jnp.bfloat16),
            pltpu.VMEM((total, 2, slab, width), jnp.bfloat16),
            pltpu.VMEM((peers, total, pot.shape[1]), f32),
        ]
        + sems,
        compiler_params=pltpu.CompilerParams(collective_id=0, has_side_effects=True, vmem_limit_bytes=48 << 20),
    )(
        *sets, proj, pot, strengths.reshape(1, -1), shifts.reshape(-1, 1),
        right[0], right[1], left[0], left[1],
    )
    return resp.transpose(2, 0, 1, 3), deriv.transpose(2, 1, 0, 3)


def solution(mesh):
    in_specs = (
        P("band", "kgrp", "pw", None),
        P("band", "kgrp", "pw", None),
        P("band", "kgrp", "pw", None),
        P("kgrp", None, "pw", None),
        P("pw", None),
        P(),
        P("band"),
    )
    out_specs = (P("band", "kgrp", "pw", None), P("band", "kgrp", "pw", None))
    def pick(*args):
        if local_plan_fits(args, mesh):
            return local_body(mesh, *args)
        return body(*args)

    return jax.shard_map(pick, mesh=mesh, in_specs=in_specs, out_specs=out_specs, check_vma=False)
```

```python
import functools
import math

import jax
import jax.numpy as jnp
import numpy as np
from jax import lax
from jax.experimental import pallas as pl
from jax.experimental.pallas import tpu as pltpu
from jax.sharding import PartitionSpec as P

ITERS = 2


precise = lax.Precision.HIGHEST
string_step = 0.05
kinetic_scale = 4.0


def margin(left_set, right_set):
    products = jnp.einsum("ixg,jyg->xyij", left_set, right_set, precision=precise)
    return jnp.stack([products[0, 0] + products[1, 1], products[0, 1] - products[1, 0]])


def combine(vectors, coeffs):
    table = jnp.stack([jnp.stack([coeffs[0], coeffs[1]]), jnp.stack([-coeffs[1], coeffs[0]])])
    return jnp.einsum("ixg,xyij->jyg", vectors, table, precision=precise)


def invert(matrix):
    real_part = matrix[0]
    imag_part = matrix[1]
    embedded = jnp.concatenate(
        [jnp.concatenate([real_part, -imag_part], 1), jnp.concatenate([imag_part, real_part], 1)], 0
    )
    normal = jnp.dot(embedded.T, embedded, precision=precise)
    lower_factor = jnp.linalg.cholesky(normal)
    middle = lax.linalg.triangular_solve(lower_factor, embedded.T, left_side=True, lower=True)
    inverse = lax.linalg.triangular_solve(
        lower_factor, middle, left_side=True, lower=True, transpose_a=True
    )
    count_rows = real_part.shape[0]
    return jnp.stack([inverse[:count_rows, :count_rows], inverse[count_rows:, :count_rows]])


def centred(index, length):
    shifted = (index + length // 2) % length - length // 2
    return shifted.astype(jnp.float32) / length


def dft_table(length, sign):
    index = jnp.arange(length, dtype=jnp.int32)
    phase = index[:, None] * index[None, :] % length
    angle = phase.astype(jnp.float32) * (2.0 * math.pi / length)
    cosine = jnp.cos(angle) / math.sqrt(length)
    sine = sign * jnp.sin(angle) / math.sqrt(length)
    return jnp.stack([jnp.stack([cosine, sine]), jnp.stack([-sine, cosine])])


def body(waves, forward, backward, projectors, potential, strengths, shifts):
    bands = waves.shape[0]
    rows = waves.shape[2]
    width = waves.shape[3]
    peers = lax.axis_size("pw")
    length = rows * peers
    points = float(length * width)
    cells = rows * width
    quarter = width // peers
    waves_flat = waves.reshape(bands, 2, cells)
    forward_flat = forward.reshape(bands, 2, cells)
    backward_flat = backward.reshape(bands, 2, cells)
    offset = lax.axis_index("band") * bands
    every_wave = lax.all_gather(waves_flat, "band", axis=0, tiled=True)
    forward_part = margin(every_wave, forward_flat) / points
    backward_part = margin(every_wave, backward_flat) / points
    forward_part, backward_part = lax.psum((forward_part, backward_part), "pw")
    forward_whole, backward_whole = (
        lax.all_gather(forward_part, "band", axis=2, tiled=True),
        lax.all_gather(backward_part, "band", axis=2, tiled=True),
    )
    forward_inverse = invert(forward_whole)
    backward_inverse = -invert(backward_whole)
    forward_cols = lax.dynamic_slice_in_dim(forward_inverse, offset, bands, 2)
    backward_cols = lax.dynamic_slice_in_dim(backward_inverse, offset, bands, 2)
    moved = combine(
        lax.all_gather(forward_flat, "band", axis=0, tiled=True), forward_cols
    ) + combine(lax.all_gather(backward_flat, "band", axis=0, tiled=True), backward_cols)
    derivative = (moved / (2.0 * string_step)).reshape(bands, 2, rows, width)
    first_index = lax.axis_index("pw") * rows + jnp.arange(rows, dtype=jnp.int32)
    second_index = jnp.arange(width, dtype=jnp.int32)
    first_freq = centred(first_index, length)
    second_freq = centred(second_index, width)
    kinetic = kinetic_scale * (
        first_freq[:, None] * first_freq[:, None] + second_freq[None, :] * second_freq[None, :]
    )
    diagonal = kinetic[None, None] + shifts[:, None, None, None]
    width_out = dft_table(width, 1.0)
    width_back = dft_table(width, -1.0)
    long_out = dft_table(length, 1.0).reshape(2, 2, peers, rows, length)
    long_back = dft_table(length, -1.0).reshape(2, 2, length, peers, rows)
    projector_flat = projectors.reshape(projectors.shape[0], 2, cells)
    residual = -derivative
    direction = residual
    solution = jnp.zeros_like(residual)
    norm_now = lax.psum(jnp.sum(residual * residual, axis=(1, 2, 3)), "pw")
    for turn in range(ITERS):
        sectioned = jnp.einsum("bxrj,xyjk->ykrb", direction, width_out, precision=precise).reshape(
            2, width, rows * bands
        )
        arrived = lax.all_to_all(sectioned, "pw", split_axis=1, concat_axis=2, tiled=True).reshape(
            2, quarter, peers, rows, bands
        )
        field = jnp.einsum("xqsrb,xysrk->yqbk", arrived, long_out, precision=precise)
        weighted = field * potential[None, :, None, :]
        leaving = jnp.einsum("xqbk,xyksr->yqsrb", weighted, long_back, precision=precise).reshape(
            2, quarter, peers * rows * bands
        )
        returned = lax.all_to_all(leaving, "pw", split_axis=2, concat_axis=1, tiled=True).reshape(
            2, width, rows, bands
        )
        smooth_part = jnp.einsum("xkrb,xykj->byrj", returned, width_back, precision=precise)
        coupling = margin(projector_flat, direction.reshape(bands, 2, cells)) / points
        own_energy = jnp.sum(diagonal * direction * direction, axis=(1, 2, 3)) + jnp.sum(
            weighted * field, axis=(0, 1, 3)
        )
        coupling, own_energy = lax.psum((coupling, own_energy), "pw")
        nonlocal_part = combine(projector_flat, coupling * strengths[None, :, None]).reshape(
            direction.shape
        )
        image = diagonal * direction + smooth_part + nonlocal_part
        curvature = own_energy + points * jnp.sum(
            strengths[None, :, None] * coupling * coupling, axis=(0, 1)
        )
        image, curvature = (image, curvature)
        alpha = (norm_now / curvature)[:, None, None, None]
        solution = solution + alpha * direction
        if turn + 1 < ITERS:
            residual = residual - alpha * image
            norm_next = lax.psum(jnp.sum(residual * residual, axis=(1, 2, 3)), "pw")
            direction = residual + (norm_next / norm_now)[:, None, None, None] * direction
            norm_now = norm_next
    return (solution, derivative)


MESH = pl.DeviceIdType.MESH
TILE = 8


def halves(x):
    high = x.astype(jnp.bfloat16)
    return high, (x - high.astype(jnp.float32)).astype(jnp.bfloat16)


def mul(a, b, turned=False):
    dims = (((1,), (1 if turned else 0,)), ((), ()))
    return lax.dot_general(a, b, dims, preferred_element_type=jnp.float32)


def mul3(a, b, turned=False):
    return mul(a[0], b[0], turned) + (mul(a[0], b[1], turned) + mul(a[1], b[0], turned))


def exact(a, b):
    return jnp.dot(a, b, precision=precise, preferred_element_type=jnp.float32)


def local_plan_fits(args, mesh):
    waves, projectors = args[0], args[3]
    peers, groups = mesh.shape["pw"], mesh.shape["band"]
    bands, rows, width = waves.shape[0], waves.shape[2], waves.shape[3]
    return (
        groups == 4
        and rows == groups
        and bands == TILE * peers
        and bands * groups == 128
        and projectors.shape[0] == 128
        and peers * rows == 16
        and width % 128 == 0
        and projectors.size * peers * 4 <= 8 << 20
    )


def local_kernel(
    peers, groups, waves, ahead, behind, proj, pot, strengths, shifts, right_hi, right_lo, left_hi, left_lo,
    resp, deriv,
    got, marg, pair, merged, parts, whole, inv, both, made, field, answer, far, phi, plo, levels,
    s_send, s_recv, m_send, m_recv, r_send, r_recv, g_send, g_recv, t_send, t_recv,
    p1_send, p1_recv, p2_send, p2_recv, p3_send, p3_recv, v_send, v_recv,
    x_send, x_recv, d_send, d_recv, o_send, o_recv,
):
    sets = (waves, ahead, behind)
    kgrp = lax.axis_index("kgrp")
    p = lax.axis_index("pw")
    b = lax.axis_index("band")
    core = lax.rem(b, 2)
    side = b // 2
    total = peers * groups
    mine = p * groups + b
    slot = p * 2 + side
    width = waves.shape[3]
    slab = groups * waves.shape[2]
    points = float(total * width)
    barrier = pltpu.get_barrier_semaphore()

    def flat(o):
        q = lax.rem(mine + o, total)
        return q // groups, lax.rem(q, groups)

    for o in range(1, total):
        q, c = flat(o)
        pl.semaphore_signal(barrier, inc=1, device_id=(kgrp, q, c), device_id_type=MESH)
    pl.semaphore_wait(barrier, total - 1)

    started = []

    def send(source, target, ssem, rsem, q, c):
        copy = pltpu.make_async_remote_copy(
            src_ref=source, dst_ref=target, send_sem=ssem, recv_sem=rsem,
            device_id=(kgrp, q, c), device_id_type=MESH,
        )
        copy.start()
        started.append(copy)
        return copy

    first = []
    for a in range(3):
        for o in range(1, groups):
            c = lax.rem(b + o, groups)
            k = a * groups + o
            first.append(send(sets[a].at[c], got.at[a, b], s_send.at[k], s_recv.at[k], p, c))
    pots, pass1, pass2, pass3 = [], [], [], []
    across = lax.rem(b + 2, groups)
    sibling = side * 2 + 1 - core
    for o in range(1, peers):
        q = lax.rem(p + o, peers)
        pots.append(send(pot, levels.at[p], v_send.at[o], v_recv.at[o], q, b))

    cut = slab * 11 // 16 // TILE * TILE
    chunks = (pl.ds(0, cut), pl.ds(cut, slab - cut))

    def spread_half(half):
        for o in range(1, peers):
            q = lax.rem(p + o, peers)
            k = half * peers + o
            pass1.append(send(proj.at[b, :, chunks[half]], far.at[mine, :, chunks[half]], p1_send.at[k], p1_recv.at[k], q, b))

    def cross_half(half):
        for o in range(1, peers):
            row = lax.rem(p + o, peers) * groups + b
            k = half * peers + o
            pass2.append(send(far.at[row, :, chunks[half]], far.at[row, :, chunks[half]], p2_send.at[k], p2_recv.at[k], p, across))

    def share_rows(j):
        for o in range(1, peers):
            row = lax.rem(p + o, peers) * groups + (b if j == 0 else across)
            k = 2 * o + j
            pass3.append(send(far.at[row], far.at[row], p3_send.at[k], p3_recv.at[k], p, sibling))

    spread_half(0)
    for a in range(3):
        got[a, b] = sets[a][b]
    levels[p] = pot[...]

    def set_of(a):
        return got[a, :, 0].reshape(slab, width), got[a, :, 1].reshape(slab, width)

    for copy in first[:3]:
        copy.wait_recv()
    wr, wi = set_of(0)
    lhs = halves(
        jnp.concatenate(
            [jnp.concatenate([wr, wi], 1), jnp.concatenate([-wi, wr], 1)], 0
        )
        * (1.0 / points)
    )
    for m in range(2):
        for copy in first[3 * m + 3 : 3 * m + 6]:
            copy.wait_recv()
        fr, fi = set_of(m + 1)
        part = mul3(lhs, halves(jnp.concatenate([fr, fi], 1)), True)
        marg[m] = part.reshape(marg.shape[1:])
    joined = send(marg.at[1 - core], pair, m_send, m_recv, p, sibling)
    joined.wait_recv()
    merged[...] = marg[core] + pair[...]
    second = []
    size = total // 2
    for o in range(1, size):
        s = lax.rem(slot + o, size)
        second.append(
            send(merged.at[s], parts.at[slot], r_send.at[o], r_recv.at[o], s // 2, lax.rem(s, 2) * 2 + core)
        )
    parts[slot] = merged[slot]

    def own_rows(r, carry):
        hi, lo = halves(proj[r])
        phi[p * groups + r] = hi
        plo[p * groups + r] = lo
        return carry

    lax.fori_loop(0, groups, own_rows, 0)
    for copy in second:
        copy.wait_recv()
    summed = parts[0]
    for k in range(1, size):
        summed = summed + parts[k]
    whole[slot] = summed
    third = []
    for o in range(1, size):
        s = lax.rem(slot + o, size)
        third.append(
            send(whole.at[slot], whole.at[slot], g_send.at[o], g_recv.at[o], s // 2, lax.rem(s, 2) * 2 + core)
        )
    for copy in pass1[: peers - 1]:
        copy.wait_recv()
    cross_half(0)
    spread_half(1)
    for copy in third:
        copy.wait_recv()
    stacked = whole[...].reshape(2 * slab, slab)
    ar, ai = stacked[:slab], stacked[slab:]
    turned = stacked.T
    inv[0] = exact(turned, stacked)
    inv[1] = exact(turned, jnp.concatenate([ai, -ar], 0))
    lane = lax.broadcasted_iota(jnp.int32, (slab, slab), 1)
    line = lax.broadcasted_iota(jnp.int32, (slab, slab), 0)
    lane1 = lax.broadcasted_iota(jnp.int32, (1, slab), 1)
    line1 = lax.broadcasted_iota(jnp.int32, (slab, 1), 0)

    def eliminate(k, carry):
        nr, ni = inv[0], inv[1]
        rr, ri = inv[0, pl.ds(k, 1), :], inv[1, pl.ds(k, 1), :]
        hit = lane == k
        cr = jnp.sum(jnp.where(hit, nr, 0.0), 1, keepdims=True)
        ci = jnp.sum(jnp.where(hit, ni, 0.0), 1, keepdims=True)
        own = lane1 == k
        scale = 1.0 / jnp.sum(jnp.where(own, rr, 0.0), 1, keepdims=True)
        sr = jnp.where(own, 1.0, rr) * scale
        si = jnp.where(own, 0.0, ri) * scale
        cr = jnp.where(line1 == k, -1.0, cr)
        ci = jnp.where(line1 == k, 0.0, ci)
        gone = jnp.logical_or(hit, line == k)
        inv[0] = jnp.where(gone, 0.0, nr) - (cr * sr - ci * si)
        inv[1] = jnp.where(gone, 0.0, ni) - (cr * si + ci * sr)
        return carry

    lax.fori_loop(0, slab // 2, eliminate, 0)
    for copy in pass1[peers - 1 :]:
        copy.wait_recv()
    cross_half(1)
    share_rows(0)
    lax.fori_loop(slab // 2, slab, eliminate, 0)
    kr, ki = inv[0], inv[1]
    mixed = exact(
        jnp.concatenate([jnp.concatenate([ar, -ai], 1), jnp.concatenate([-ai, -ar], 1)], 0),
        jnp.concatenate([kr, ki], 0),
    )
    sign = (1 - 2 * core).astype(jnp.float32) / (2.0 * string_step)
    both[core] = mixed * sign
    swap = send(both.at[core], both.at[core], t_send, t_recv, p, sibling)
    for copy in pass2:
        copy.wait_recv()
    share_rows(1)
    fr, fi = set_of(1)
    br, bi = set_of(2)
    rhs = halves(jnp.concatenate([fr, fi, br, bi], 0))
    swap.wait_recv()
    f, g = both[0], both[1]
    tfr, tfi, tbr, tbi = f[:slab], f[slab:], g[:slab], g[slab:]
    table = halves(
        jnp.concatenate(
            [
                jnp.concatenate([tfr, -tfi, tbr, -tbi], 1),
                jnp.concatenate([tfi, tfr, tbi, tbr], 1),
            ],
            0,
        )
    )
    made[...] = mul3(table, rhs).reshape(made.shape)
    fields, outs = [], []
    for o in range(1, total):
        q, c = flat(o)
        rows = pl.ds(pl.multiple_of((c * peers + q) * TILE, TILE), TILE)
        fields.append(send(made.at[:, rows], field.at[:, mine], x_send.at[o], x_recv.at[o], q, c))
    span = slab // groups
    for o in range(1, groups):
        c = lax.rem(b + o, groups)
        rows = pl.ds(pl.multiple_of(c * span, TILE), span)
        outs.append(send(made.at[:, rows], deriv.at[b], d_send.at[o], d_recv.at[o], p, c))
    field[:, mine] = made[:, pl.ds(pl.multiple_of((b * peers + p) * TILE, TILE), TILE)]
    deriv[b] = made[:, pl.ds(pl.multiple_of(b * span, TILE), span)]
    for copy in pass3:
        copy.wait_recv()

    def far_rows(t, carry):
        row = lax.rem(p * groups + groups + t, total)
        hi, lo = halves(far[row])
        phi[row] = hi
        plo[row] = lo
        return carry

    lax.fori_loop(0, total - groups, far_rows, 0)
    for copy in pots:
        copy.wait_recv()
    share = width // peers
    level = jnp.concatenate([levels[k][:, :share] for k in range(peers)], 1)
    level = jnp.broadcast_to(level[:, None, :], (total, TILE, width)).reshape(total * TILE, width)
    iu = lax.broadcasted_iota(jnp.int32, (total, TILE, width), 0)
    iw = lax.broadcasted_iota(jnp.int32, (total, TILE, width), 2)
    fu = jnp.where(iu < total // 2, iu, iu - total).astype(jnp.float32) / total
    fw = jnp.where(iw < width // 2, iw, iw - width).astype(jnp.float32) / width
    shift = shifts[pl.ds(pl.multiple_of(p * TILE, TILE), TILE), :]
    diagonal = kinetic_scale * (fu * fu + fw * fw) + shift[None]
    diagonal = diagonal.reshape(total * TILE, width)
    for copy in fields:
        copy.wait_recv()

    def transform(xr, xi):
        y = mul3(halves(jnp.concatenate([xr, xi], 1)), (right_hi[...], right_lo[...]))
        y = jnp.concatenate([y[:, :width], y[:, width:]], 0)
        z = mul3((left_hi[...], left_lo[...]), halves(y))
        return z[: total * TILE], z[total * TILE :]

    def energy(dr, di):
        yr, yi = transform(dr, di)
        coupling = project(dr, di)
        local = summed_over(diagonal * (dr * dr + di * di) + level * (yr * yr + yi * yi))
        weight = jnp.sum(coupling * coupling * strengths[...], 1, keepdims=True) * points
        return local + weight[:TILE] + weight[TILE:]

    def project(dr, di):
        accr = jnp.zeros((2 * TILE, slab), jnp.float32)
        acci = jnp.zeros((2 * TILE, slab), jnp.float32)
        for i in range(total):
            at = slice(i * TILE, i * TILE + TILE)
            hi, lo = halves(jnp.concatenate([dr[at], di[at]], 0))
            accr = accr + mul3((hi, lo), (phi[i, 0], plo[i, 0]), True)
            acci = acci + mul3((hi, lo), (phi[i, 1], plo[i, 1]), True)
        return jnp.concatenate(
            [accr[:TILE] + acci[TILE:], accr[TILE:] - acci[:TILE]], 0
        ) * (1.0 / points)

    def operate(dr, di):
        yr, yi = transform(dr, di)
        zr, zi = transform(yr * level, -(yi * level))
        c2 = halves(project(dr, di) * strengths[...])
        outr, outi = [], []
        for i in range(total):
            ur = mul3(c2, (phi[i, 0], plo[i, 0]))
            ui = mul3(c2, (phi[i, 1], plo[i, 1]))
            outr.append(ur[:TILE] - ui[TILE:])
            outi.append(ui[:TILE] + ur[TILE:])
        return (
            diagonal * dr + zr + jnp.concatenate(outr, 0),
            diagonal * di - zi + jnp.concatenate(outi, 0),
        )

    def summed_over(x):
        x = x.reshape(total, TILE, width)
        return jnp.sum(jnp.sum(x, 0), 1, keepdims=True)

    def spread(x):
        return jnp.broadcast_to(x[None], (total, TILE, width)).reshape(total * TILE, width)

    rr = -field[0].reshape(total * TILE, width)
    ri = -field[1].reshape(total * TILE, width)
    dr, di = rr, ri
    norm_now = summed_over(rr * rr + ri * ri)
    solr, soli = jnp.zeros_like(dr), jnp.zeros_like(di)
    for turn in range(ITERS):
        if turn + 1 < ITERS:
            imr, imi = operate(dr, di)
            curvature = summed_over(dr * imr + di * imi)
        else:
            curvature = energy(dr, di)
        alpha = spread(norm_now / curvature)
        solr, soli = solr + alpha * dr, soli + alpha * di
        if turn + 1 < ITERS:
            rr, ri = rr - alpha * imr, ri - alpha * imi
            norm_next = summed_over(rr * rr + ri * ri)
            beta = spread(norm_next / norm_now)
            dr, di = rr + beta * dr, ri + beta * di
            norm_now = norm_next
    answer[0] = solr.reshape(total, TILE, width)
    answer[1] = soli.reshape(total, TILE, width)
    here = pl.ds(pl.multiple_of(p * TILE, TILE), TILE)
    for o in range(1, peers):
        q = lax.rem(p + o, peers)
        outs.append(
            send(answer.at[:, pl.ds(q * groups, groups)], resp.at[:, :, here], o_send.at[o], o_recv.at[o], q, b)
        )
    resp[:, :, here] = answer[:, pl.ds(p * groups, groups)]
    for copy in outs:
        copy.wait_recv()
    for copy in started:
        copy.wait_send()


def tables(length, repeat):
    index = np.arange(length)
    angle = (index[:, None] * index[None, :] % length) * (2.0 * math.pi / length)
    eye = np.eye(repeat)
    cosine = np.kron(np.cos(angle) / math.sqrt(length), eye)
    sine = np.kron(np.sin(angle) / math.sqrt(length), eye)
    return cosine.astype(np.float32), sine.astype(np.float32)


def split_table(table):
    return halves(jnp.asarray(table))


def local_body(mesh, waves, forward, backward, projectors, potential, strengths, shifts):
    peers, groups = mesh.shape["pw"], mesh.shape["band"]
    bands, _, rows, width = waves.shape
    slab, total = bands * groups, peers * rows
    sets = [x.transpose(2, 1, 0, 3) for x in (waves, forward, backward)]
    proj = projectors.transpose(2, 1, 0, 3)
    pot = jnp.pad(potential.T, ((0, 0), (0, 128 - potential.shape[0] % 128)))
    c, s = tables(width, 1)
    right = split_table(np.block([[c, s], [-s, c]]))
    c, s = tables(total, TILE)
    left = split_table(np.block([[c, -s], [s, c]]))
    f32 = jnp.float32
    dma = pltpu.SemaphoreType.DMA
    vmem = pl.BlockSpec(memory_space=pltpu.VMEM)
    sems = []
    for count in ((3 * groups,), (), (total // 2,), (total // 2,), ()):
        sems += [dma(count) if count else dma, dma(count) if count else dma]
    for count in (2 * peers, 2 * peers, 2 * peers, peers, total, groups, peers):
        sems += [dma((count,)), dma((count,))]
    resp, deriv = pl.pallas_call(
        functools.partial(local_kernel, peers, groups),
        out_shape=(
            jax.ShapeDtypeStruct((2, rows, bands, width), f32),
            jax.ShapeDtypeStruct((rows, 2, bands, width), f32),
        ),
        in_specs=[vmem] * 11,
        out_specs=(vmem, vmem),
        scratch_shapes=[
            pltpu.VMEM((3, groups, 2, bands, width), f32),
            pltpu.VMEM((2, total // 2, 4 * slab // total, slab), f32),
            pltpu.VMEM((total // 2, 4 * slab // total, slab), f32),
            pltpu.VMEM((total // 2, 4 * slab // total, slab), f32),
            pltpu.VMEM((total // 2, 4 * slab // total, slab), f32),
            pltpu.VMEM((total // 2, 4 * slab // total, slab), f32),
            pltpu.VMEM((2, slab, slab), f32),
            pltpu.VMEM((2, 2 * slab, slab), f32),
            pltpu.VMEM((2, slab, width), f32),
            pltpu.VMEM((2, total, TILE, width), f32),
            pltpu.VMEM((2, total, TILE, width), f32),
            pltpu.VMEM((total, 2, slab, width), f32),
            pltpu.VMEM((total, 2, slab, width), jnp.bfloat16),
            pltpu.VMEM((total, 2, slab, width), jnp.bfloat16),
            pltpu.VMEM((peers, total, pot.shape[1]), f32),
        ]
        + sems,
        compiler_params=pltpu.CompilerParams(collective_id=0, has_side_effects=True, vmem_limit_bytes=48 << 20),
    )(
        *sets, proj, pot, strengths.reshape(1, -1), shifts.reshape(-1, 1),
        right[0], right[1], left[0], left[1],
    )
    return resp.transpose(2, 0, 1, 3), deriv.transpose(2, 1, 0, 3)


def solution(mesh):
    in_specs = (
        P("band", "kgrp", "pw", None),
        P("band", "kgrp", "pw", None),
        P("band", "kgrp", "pw", None),
        P("kgrp", None, "pw", None),
        P("pw", None),
        P(),
        P("band"),
    )
    out_specs = (P("band", "kgrp", "pw", None), P("band", "kgrp", "pw", None))
    def pick(*args):
        if local_plan_fits(args, mesh):
            return local_body(mesh, *args)
        return body(*args)

    return jax.shard_map(pick, mesh=mesh, in_specs=in_specs, out_specs=out_specs, check_vma=False)
```

```python
import functools
import math

import jax
import jax.numpy as jnp
import numpy as np
from jax import lax
from jax.experimental import pallas as pl
from jax.experimental.pallas import tpu as pltpu
from jax.sharding import PartitionSpec as P

ITERS = 2


precise = lax.Precision.HIGHEST
string_step = 0.05
kinetic_scale = 4.0


def margin(left_set, right_set):
    products = jnp.einsum("ixg,jyg->xyij", left_set, right_set, precision=precise)
    return jnp.stack([products[0, 0] + products[1, 1], products[0, 1] - products[1, 0]])


def combine(vectors, coeffs):
    table = jnp.stack([jnp.stack([coeffs[0], coeffs[1]]), jnp.stack([-coeffs[1], coeffs[0]])])
    return jnp.einsum("ixg,xyij->jyg", vectors, table, precision=precise)


def invert(matrix):
    real_part = matrix[0]
    imag_part = matrix[1]
    embedded = jnp.concatenate(
        [jnp.concatenate([real_part, -imag_part], 1), jnp.concatenate([imag_part, real_part], 1)], 0
    )
    normal = jnp.dot(embedded.T, embedded, precision=precise)
    lower_factor = jnp.linalg.cholesky(normal)
    middle = lax.linalg.triangular_solve(lower_factor, embedded.T, left_side=True, lower=True)
    inverse = lax.linalg.triangular_solve(
        lower_factor, middle, left_side=True, lower=True, transpose_a=True
    )
    count_rows = real_part.shape[0]
    return jnp.stack([inverse[:count_rows, :count_rows], inverse[count_rows:, :count_rows]])


def centred(index, length):
    shifted = (index + length // 2) % length - length // 2
    return shifted.astype(jnp.float32) / length


def dft_table(length, sign):
    index = jnp.arange(length, dtype=jnp.int32)
    phase = index[:, None] * index[None, :] % length
    angle = phase.astype(jnp.float32) * (2.0 * math.pi / length)
    cosine = jnp.cos(angle) / math.sqrt(length)
    sine = sign * jnp.sin(angle) / math.sqrt(length)
    return jnp.stack([jnp.stack([cosine, sine]), jnp.stack([-sine, cosine])])


def body(waves, forward, backward, projectors, potential, strengths, shifts):
    bands = waves.shape[0]
    rows = waves.shape[2]
    width = waves.shape[3]
    peers = lax.axis_size("pw")
    length = rows * peers
    points = float(length * width)
    cells = rows * width
    quarter = width // peers
    waves_flat = waves.reshape(bands, 2, cells)
    forward_flat = forward.reshape(bands, 2, cells)
    backward_flat = backward.reshape(bands, 2, cells)
    offset = lax.axis_index("band") * bands
    every_wave = lax.all_gather(waves_flat, "band", axis=0, tiled=True)
    forward_part = margin(every_wave, forward_flat) / points
    backward_part = margin(every_wave, backward_flat) / points
    forward_part, backward_part = lax.psum((forward_part, backward_part), "pw")
    forward_whole, backward_whole = (
        lax.all_gather(forward_part, "band", axis=2, tiled=True),
        lax.all_gather(backward_part, "band", axis=2, tiled=True),
    )
    forward_inverse = invert(forward_whole)
    backward_inverse = -invert(backward_whole)
    forward_cols = lax.dynamic_slice_in_dim(forward_inverse, offset, bands, 2)
    backward_cols = lax.dynamic_slice_in_dim(backward_inverse, offset, bands, 2)
    moved = combine(
        lax.all_gather(forward_flat, "band", axis=0, tiled=True), forward_cols
    ) + combine(lax.all_gather(backward_flat, "band", axis=0, tiled=True), backward_cols)
    derivative = (moved / (2.0 * string_step)).reshape(bands, 2, rows, width)
    first_index = lax.axis_index("pw") * rows + jnp.arange(rows, dtype=jnp.int32)
    second_index = jnp.arange(width, dtype=jnp.int32)
    first_freq = centred(first_index, length)
    second_freq = centred(second_index, width)
    kinetic = kinetic_scale * (
        first_freq[:, None] * first_freq[:, None] + second_freq[None, :] * second_freq[None, :]
    )
    diagonal = kinetic[None, None] + shifts[:, None, None, None]
    width_out = dft_table(width, 1.0)
    width_back = dft_table(width, -1.0)
    long_out = dft_table(length, 1.0).reshape(2, 2, peers, rows, length)
    long_back = dft_table(length, -1.0).reshape(2, 2, length, peers, rows)
    projector_flat = projectors.reshape(projectors.shape[0], 2, cells)
    residual = -derivative
    direction = residual
    solution = jnp.zeros_like(residual)
    norm_now = lax.psum(jnp.sum(residual * residual, axis=(1, 2, 3)), "pw")
    for turn in range(ITERS):
        sectioned = jnp.einsum("bxrj,xyjk->ykrb", direction, width_out, precision=precise).reshape(
            2, width, rows * bands
        )
        arrived = lax.all_to_all(sectioned, "pw", split_axis=1, concat_axis=2, tiled=True).reshape(
            2, quarter, peers, rows, bands
        )
        field = jnp.einsum("xqsrb,xysrk->yqbk", arrived, long_out, precision=precise)
        weighted = field * potential[None, :, None, :]
        leaving = jnp.einsum("xqbk,xyksr->yqsrb", weighted, long_back, precision=precise).reshape(
            2, quarter, peers * rows * bands
        )
        returned = lax.all_to_all(leaving, "pw", split_axis=2, concat_axis=1, tiled=True).reshape(
            2, width, rows, bands
        )
        smooth_part = jnp.einsum("xkrb,xykj->byrj", returned, width_back, precision=precise)
        coupling = margin(projector_flat, direction.reshape(bands, 2, cells)) / points
        own_energy = jnp.sum(diagonal * direction * direction, axis=(1, 2, 3)) + jnp.sum(
            weighted * field, axis=(0, 1, 3)
        )
        coupling, own_energy = lax.psum((coupling, own_energy), "pw")
        nonlocal_part = combine(projector_flat, coupling * strengths[None, :, None]).reshape(
            direction.shape
        )
        image = diagonal * direction + smooth_part + nonlocal_part
        curvature = own_energy + points * jnp.sum(
            strengths[None, :, None] * coupling * coupling, axis=(0, 1)
        )
        image, curvature = (image, curvature)
        alpha = (norm_now / curvature)[:, None, None, None]
        solution = solution + alpha * direction
        if turn + 1 < ITERS:
            residual = residual - alpha * image
            norm_next = lax.psum(jnp.sum(residual * residual, axis=(1, 2, 3)), "pw")
            direction = residual + (norm_next / norm_now)[:, None, None, None] * direction
            norm_now = norm_next
    return (solution, derivative)


MESH = pl.DeviceIdType.MESH
TILE = 8


def halves(x):
    high = x.astype(jnp.bfloat16)
    return high, (x - high.astype(jnp.float32)).astype(jnp.bfloat16)


def mul(a, b, turned=False):
    dims = (((1,), (1 if turned else 0,)), ((), ()))
    return lax.dot_general(a, b, dims, preferred_element_type=jnp.float32)


def mul3(a, b, turned=False):
    return mul(a[0], b[0], turned) + (mul(a[0], b[1], turned) + mul(a[1], b[0], turned))


def exact(a, b):
    return jnp.dot(a, b, precision=precise, preferred_element_type=jnp.float32)


def local_plan_fits(args, mesh):
    waves, projectors = args[0], args[3]
    peers, groups = mesh.shape["pw"], mesh.shape["band"]
    bands, rows, width = waves.shape[0], waves.shape[2], waves.shape[3]
    return (
        groups == 4
        and rows == groups
        and bands == TILE * peers
        and bands * groups == 128
        and projectors.shape[0] == 128
        and peers * rows == 16
        and width % 128 == 0
        and projectors.size * peers * 4 <= 8 << 20
    )


def local_kernel(
    peers, groups, waves, ahead, behind, proj, pot, strengths, shifts, right_hi, right_lo, left_hi, left_lo,
    resp, deriv,
    got, marg, pair, merged, parts, whole, inv, both, made, field, answer, far, phi, plo, levels,
    s_send, s_recv, m_send, m_recv, r_send, r_recv, g_send, g_recv, t_send, t_recv,
    p1_send, p1_recv, p2_send, p2_recv, p3_send, p3_recv, v_send, v_recv,
    x_send, x_recv, d_send, d_recv, o_send, o_recv,
):
    sets = (waves, ahead, behind)
    kgrp = lax.axis_index("kgrp")
    p = lax.axis_index("pw")
    b = lax.axis_index("band")
    core = lax.rem(b, 2)
    side = b // 2
    total = peers * groups
    mine = p * groups + b
    slot = p * 2 + side
    width = waves.shape[3]
    slab = groups * waves.shape[2]
    points = float(total * width)
    barrier = pltpu.get_barrier_semaphore()

    def flat(o):
        q = lax.rem(mine + o, total)
        return q // groups, lax.rem(q, groups)

    for o in range(1, total):
        q, c = flat(o)
        pl.semaphore_signal(barrier, inc=1, device_id=(kgrp, q, c), device_id_type=MESH)
    pl.semaphore_wait(barrier, total - 1)

    started = []

    def send(source, target, ssem, rsem, q, c):
        copy = pltpu.make_async_remote_copy(
            src_ref=source, dst_ref=target, send_sem=ssem, recv_sem=rsem,
            device_id=(kgrp, q, c), device_id_type=MESH,
        )
        copy.start()
        started.append(copy)
        return copy

    first = []
    for a in range(3):
        for o in range(1, groups):
            c = lax.rem(b + o, groups)
            k = a * groups + o
            first.append(send(sets[a].at[c], got.at[a, b], s_send.at[k], s_recv.at[k], p, c))
    pots, pass1, pass2, pass3 = [], [], [], []
    across = lax.rem(b + 2, groups)
    sibling = side * 2 + 1 - core
    for o in range(1, peers):
        q = lax.rem(p + o, peers)
        pots.append(send(pot, levels.at[p], v_send.at[o], v_recv.at[o], q, b))

    cut = slab // 2 // TILE * TILE
    chunks = (pl.ds(0, cut), pl.ds(cut, slab - cut))

    def spread_half(half):
        for o in range(1, peers):
            q = lax.rem(p + o, peers)
            k = half * peers + o
            pass1.append(send(proj.at[b, :, chunks[half]], far.at[mine, :, chunks[half]], p1_send.at[k], p1_recv.at[k], q, b))

    def cross_half(half):
        for o in range(1, peers):
            row = lax.rem(p + o, peers) * groups + b
            k = half * peers + o
            pass2.append(send(far.at[row, :, chunks[half]], far.at[row, :, chunks[half]], p2_send.at[k], p2_recv.at[k], p, across))

    def share_rows(j):
        for o in range(1, peers):
            row = lax.rem(p + o, peers) * groups + (b if j == 0 else across)
            k = 2 * o + j
            pass3.append(send(far.at[row], far.at[row], p3_send.at[k], p3_recv.at[k], p, sibling))

    spread_half(0)
    for a in range(3):
        got[a, b] = sets[a][b]
    levels[p] = pot[...]

    def set_of(a):
        return got[a, :, 0].reshape(slab, width), got[a, :, 1].reshape(slab, width)

    for copy in first[:3]:
        copy.wait_recv()
    wr, wi = set_of(0)
    lhs = halves(
        jnp.concatenate(
            [jnp.concatenate([wr, wi], 1), jnp.concatenate([-wi, wr], 1)], 0
        )
        * (1.0 / points)
    )
    for m in range(2):
        for copy in first[3 * m + 3 : 3 * m + 6]:
            copy.wait_recv()
        fr, fi = set_of(m + 1)
        part = mul3(lhs, halves(jnp.concatenate([fr, fi], 1)), True)
        marg[m] = part.reshape(marg.shape[1:])
    joined = send(marg.at[1 - core], pair, m_send, m_recv, p, sibling)
    joined.wait_recv()
    merged[...] = marg[core] + pair[...]
    second = []
    size = total // 2
    for o in range(1, size):
        s = lax.rem(slot + o, size)
        second.append(
            send(merged.at[s], parts.at[slot], r_send.at[o], r_recv.at[o], s // 2, lax.rem(s, 2) * 2 + core)
        )
    parts[slot] = merged[slot]

    def own_rows(r, carry):
        hi, lo = halves(proj[r])
        phi[p * groups + r] = hi
        plo[p * groups + r] = lo
        return carry

    lax.fori_loop(0, groups, own_rows, 0)
    for copy in second:
        copy.wait_recv()
    summed = parts[0]
    for k in range(1, size):
        summed = summed + parts[k]
    whole[slot] = summed
    third = []
    for o in range(1, size):
        s = lax.rem(slot + o, size)
        third.append(
            send(whole.at[slot], whole.at[slot], g_send.at[o], g_recv.at[o], s // 2, lax.rem(s, 2) * 2 + core)
        )
    for copy in pass1[: peers - 1]:
        copy.wait_recv()
    cross_half(0)
    spread_half(1)
    for copy in third:
        copy.wait_recv()
    stacked = whole[...].reshape(2 * slab, slab)
    ar, ai = stacked[:slab], stacked[slab:]
    turned = stacked.T
    inv[0] = exact(turned, stacked)
    inv[1] = exact(turned, jnp.concatenate([ai, -ar], 0))
    lane = lax.broadcasted_iota(jnp.int32, (slab, slab), 1)
    line = lax.broadcasted_iota(jnp.int32, (slab, slab), 0)
    lane1 = lax.broadcasted_iota(jnp.int32, (1, slab), 1)
    line1 = lax.broadcasted_iota(jnp.int32, (slab, 1), 0)

    def eliminate(k, carry):
        nr, ni = inv[0], inv[1]
        rr, ri = inv[0, pl.ds(k, 1), :], inv[1, pl.ds(k, 1), :]
        hit = lane == k
        cr = jnp.sum(jnp.where(hit, nr, 0.0), 1, keepdims=True)
        ci = jnp.sum(jnp.where(hit, ni, 0.0), 1, keepdims=True)
        own = lane1 == k
        scale = 1.0 / jnp.sum(jnp.where(own, rr, 0.0), 1, keepdims=True)
        sr = jnp.where(own, 1.0, rr) * scale
        si = jnp.where(own, 0.0, ri) * scale
        cr = jnp.where(line1 == k, -1.0, cr)
        ci = jnp.where(line1 == k, 0.0, ci)
        gone = jnp.logical_or(hit, line == k)
        inv[0] = jnp.where(gone, 0.0, nr) - (cr * sr - ci * si)
        inv[1] = jnp.where(gone, 0.0, ni) - (cr * si + ci * sr)
        return carry

    lax.fori_loop(0, slab * 5 // 8, eliminate, 0, unroll=4)
    for copy in pass1[peers - 1 :]:
        copy.wait_recv()
    cross_half(1)
    share_rows(0)
    lax.fori_loop(slab * 5 // 8, slab, eliminate, 0, unroll=4)
    kr, ki = inv[0], inv[1]
    mixed = exact(
        jnp.concatenate([jnp.concatenate([ar, -ai], 1), jnp.concatenate([-ai, -ar], 1)], 0),
        jnp.concatenate([kr, ki], 0),
    )
    sign = (1 - 2 * core).astype(jnp.float32) / (2.0 * string_step)
    both[core] = mixed * sign
    swap = send(both.at[core], both.at[core], t_send, t_recv, p, sibling)
    for copy in pass2:
        copy.wait_recv()
    share_rows(1)
    fr, fi = set_of(1)
    br, bi = set_of(2)
    rhs = halves(jnp.concatenate([fr, fi, br, bi], 0))
    swap.wait_recv()
    f, g = both[0], both[1]
    tfr, tfi, tbr, tbi = f[:slab], f[slab:], g[:slab], g[slab:]
    table = halves(
        jnp.concatenate(
            [
                jnp.concatenate([tfr, -tfi, tbr, -tbi], 1),
                jnp.concatenate([tfi, tfr, tbi, tbr], 1),
            ],
            0,
        )
    )
    made[...] = mul3(table, rhs).reshape(made.shape)
    fields, outs = [], []
    for o in range(1, total):
        q, c = flat(o)
        rows = pl.ds(pl.multiple_of((c * peers + q) * TILE, TILE), TILE)
        fields.append(send(made.at[:, rows], field.at[:, mine], x_send.at[o], x_recv.at[o], q, c))
    span = slab // groups
    for o in range(1, groups):
        c = lax.rem(b + o, groups)
        rows = pl.ds(pl.multiple_of(c * span, TILE), span)
        outs.append(send(made.at[:, rows], deriv.at[b], d_send.at[o], d_recv.at[o], p, c))
    field[:, mine] = made[:, pl.ds(pl.multiple_of((b * peers + p) * TILE, TILE), TILE)]
    deriv[b] = made[:, pl.ds(pl.multiple_of(b * span, TILE), span)]
    for copy in pass3:
        copy.wait_recv()

    def far_rows(t, carry):
        row = lax.rem(p * groups + groups + t, total)
        hi, lo = halves(far[row])
        phi[row] = hi
        plo[row] = lo
        return carry

    lax.fori_loop(0, total - groups, far_rows, 0)
    for copy in pots:
        copy.wait_recv()
    level = jnp.concatenate([levels[k] for k in range(peers)], 1)
    level = jnp.broadcast_to(level[:, None, :], (total, TILE, width)).reshape(total * TILE, width)
    iu = lax.broadcasted_iota(jnp.int32, (total, TILE, width), 0)
    iw = lax.broadcasted_iota(jnp.int32, (total, TILE, width), 2)
    fu = jnp.where(iu < total // 2, iu, iu - total).astype(jnp.float32) / total
    fw = jnp.where(iw < width // 2, iw, iw - width).astype(jnp.float32) / width
    shift = shifts[pl.ds(pl.multiple_of(p * TILE, TILE), TILE), :]
    diagonal = kinetic_scale * (fu * fu + fw * fw) + shift[None]
    diagonal = diagonal.reshape(total * TILE, width)
    for copy in fields:
        copy.wait_recv()

    def transform(xr, xi):
        y = mul3(halves(jnp.concatenate([xr, xi], 1)), (right_hi[...], right_lo[...]))
        y = jnp.concatenate([y[:, :width], y[:, width:]], 0)
        z = mul3((left_hi[...], left_lo[...]), halves(y))
        return z[: total * TILE], z[total * TILE :]

    def energy(dr, di):
        yr, yi = transform(dr, di)
        coupling = project(dr, di)
        local = summed_over(diagonal * (dr * dr + di * di) + level * (yr * yr + yi * yi))
        weight = jnp.sum(coupling * coupling * strengths[...], 1, keepdims=True) * points
        return local + weight[:TILE] + weight[TILE:]

    def project(dr, di):
        accr = jnp.zeros((2 * TILE, slab), jnp.float32)
        acci = jnp.zeros((2 * TILE, slab), jnp.float32)
        for i in range(total):
            at = slice(i * TILE, i * TILE + TILE)
            hi, lo = halves(jnp.concatenate([dr[at], di[at]], 0))
            accr = accr + mul3((hi, lo), (phi[i, 0], plo[i, 0]), True)
            acci = acci + mul3((hi, lo), (phi[i, 1], plo[i, 1]), True)
        return jnp.concatenate(
            [accr[:TILE] + acci[TILE:], accr[TILE:] - acci[:TILE]], 0
        ) * (1.0 / points)

    def operate(dr, di):
        yr, yi = transform(dr, di)
        zr, zi = transform(yr * level, -(yi * level))
        c2 = halves(project(dr, di) * strengths[...])
        outr, outi = [], []
        for i in range(total):
            ur = mul3(c2, (phi[i, 0], plo[i, 0]))
            ui = mul3(c2, (phi[i, 1], plo[i, 1]))
            outr.append(ur[:TILE] - ui[TILE:])
            outi.append(ui[:TILE] + ur[TILE:])
        return (
            diagonal * dr + zr + jnp.concatenate(outr, 0),
            diagonal * di - zi + jnp.concatenate(outi, 0),
        )

    def summed_over(x):
        x = x.reshape(total, TILE, width)
        return jnp.sum(jnp.sum(x, 0), 1, keepdims=True)

    def spread(x):
        return jnp.broadcast_to(x[None], (total, TILE, width)).reshape(total * TILE, width)

    rr = -field[0].reshape(total * TILE, width)
    ri = -field[1].reshape(total * TILE, width)
    dr, di = rr, ri
    norm_now = summed_over(rr * rr + ri * ri)
    solr, soli = jnp.zeros_like(dr), jnp.zeros_like(di)
    for turn in range(ITERS):
        if turn + 1 < ITERS:
            imr, imi = operate(dr, di)
            curvature = summed_over(dr * imr + di * imi)
        else:
            curvature = energy(dr, di)
        alpha = spread(norm_now / curvature)
        solr, soli = solr + alpha * dr, soli + alpha * di
        if turn + 1 < ITERS:
            rr, ri = rr - alpha * imr, ri - alpha * imi
            norm_next = summed_over(rr * rr + ri * ri)
            beta = spread(norm_next / norm_now)
            dr, di = rr + beta * dr, ri + beta * di
            norm_now = norm_next
    answer[0] = solr.reshape(total, TILE, width)
    answer[1] = soli.reshape(total, TILE, width)
    here = pl.ds(pl.multiple_of(p * TILE, TILE), TILE)
    for o in range(1, peers):
        q = lax.rem(p + o, peers)
        outs.append(
            send(answer.at[:, pl.ds(q * groups, groups)], resp.at[:, :, here], o_send.at[o], o_recv.at[o], q, b)
        )
    resp[:, :, here] = answer[:, pl.ds(p * groups, groups)]
    for copy in outs:
        copy.wait_recv()
    for copy in started:
        copy.wait_send()


def tables(length, repeat):
    index = np.arange(length)
    angle = (index[:, None] * index[None, :] % length) * (2.0 * math.pi / length)
    eye = np.eye(repeat)
    cosine = np.kron(np.cos(angle) / math.sqrt(length), eye)
    sine = np.kron(np.sin(angle) / math.sqrt(length), eye)
    return cosine.astype(np.float32), sine.astype(np.float32)


def split_table(table):
    return halves(jnp.asarray(table))


def local_body(mesh, waves, forward, backward, projectors, potential, strengths, shifts):
    peers, groups = mesh.shape["pw"], mesh.shape["band"]
    bands, _, rows, width = waves.shape
    slab, total = bands * groups, peers * rows
    sets = [x.transpose(2, 1, 0, 3) for x in (waves, forward, backward)]
    proj = projectors.transpose(2, 1, 0, 3)
    pot = potential.T
    c, s = tables(width, 1)
    right = split_table(np.block([[c, s], [-s, c]]))
    c, s = tables(total, TILE)
    left = split_table(np.block([[c, -s], [s, c]]))
    f32 = jnp.float32
    dma = pltpu.SemaphoreType.DMA
    vmem = pl.BlockSpec(memory_space=pltpu.VMEM)
    sems = []
    for count in ((3 * groups,), (), (total // 2,), (total // 2,), ()):
        sems += [dma(count) if count else dma, dma(count) if count else dma]
    for count in (2 * peers, 2 * peers, 2 * peers, peers, total, groups, peers):
        sems += [dma((count,)), dma((count,))]
    resp, deriv = pl.pallas_call(
        functools.partial(local_kernel, peers, groups),
        out_shape=(
            jax.ShapeDtypeStruct((2, rows, bands, width), f32),
            jax.ShapeDtypeStruct((rows, 2, bands, width), f32),
        ),
        in_specs=[vmem] * 11,
        out_specs=(vmem, vmem),
        scratch_shapes=[
            pltpu.VMEM((3, groups, 2, bands, width), f32),
            pltpu.VMEM((2, total // 2, 4 * slab // total, slab), f32),
            pltpu.VMEM((total // 2, 4 * slab // total, slab), f32),
            pltpu.VMEM((total // 2, 4 * slab // total, slab), f32),
            pltpu.VMEM((total // 2, 4 * slab // total, slab), f32),
            pltpu.VMEM((total // 2, 4 * slab // total, slab), f32),
            pltpu.VMEM((2, slab, slab), f32),
            pltpu.VMEM((2, 2 * slab, slab), f32),
            pltpu.VMEM((2, slab, width), f32),
            pltpu.VMEM((2, total, TILE, width), f32),
            pltpu.VMEM((2, total, TILE, width), f32),
            pltpu.VMEM((total, 2, slab, width), f32),
            pltpu.VMEM((total, 2, slab, width), jnp.bfloat16),
            pltpu.VMEM((total, 2, slab, width), jnp.bfloat16),
            pltpu.VMEM((peers, total, pot.shape[1]), f32),
        ]
        + sems,
        compiler_params=pltpu.CompilerParams(collective_id=0, has_side_effects=True, vmem_limit_bytes=48 << 20),
    )(
        *sets, proj, pot, strengths.reshape(1, -1), shifts.reshape(-1, 1),
        right[0], right[1], left[0], left[1],
    )
    return resp.transpose(2, 0, 1, 3), deriv.transpose(2, 1, 0, 3)


def solution(mesh):
    in_specs = (
        P("band", "kgrp", "pw", None),
        P("band", "kgrp", "pw", None),
        P("band", "kgrp", "pw", None),
        P("kgrp", None, "pw", None),
        P("pw", None),
        P(),
        P("band"),
    )
    out_specs = (P("band", "kgrp", "pw", None), P("band", "kgrp", "pw", None))
    def pick(*args):
        if local_plan_fits(args, mesh):
            return local_body(mesh, *args)
        return body(*args)

    return jax.shard_map(pick, mesh=mesh, in_specs=in_specs, out_specs=out_specs, check_vma=False)
```
